8 devices in a mesh: dp: 1 (over z), vp: 2 (over y), tp: 4 (over x, core).
Axes of the slice: x: 2, y: 2, z: 1, core: 2. Of those that a mesh axis runs over, the one named last changes fastest.
Arguments:
- hidden: bfloat16 [64, 2048], P('dp', 'tp')
- lnf_gain: float32 [2048], P('tp')
- lnf_bias: float32 [2048], P('tp')
- emb_table: bfloat16 [250880, 2048], P('vp', 'tp')
- next_tok: int32 [64], P('dp')
- eln_gain: float32 [2048], P('tp')
- eln_bias: float32 [2048], P('tp')
Outputs:
- output 1: float32 [64, 250880], P('dp', ('vp', 'tp'))
- output 2: float32 [64], P('dp')
- output 3: bfloat16 [64, 2048], P('dp', 'tp')
All inputs are finite; a program needn't handle non-finite values.
Results may differ from the reference program's by a relative error of at most 0.001.
Values sent between devices are 32-bit elements.
A program may use at most 1 GiB of HBM per device.

```python
import jax
import jax.numpy as jnp

BATCH_ROWS = 64
D = 2048
VOCAB_SIZE = 250880
VP_BLOCKS = 2
HOT_COUNT = min(2, VP_BLOCKS)
NORM_EPS = 1e-5


def draw_tokens(key):
    key_hot, key_pick, key_any, key_sel, key_pos = jax.random.split(key, 5)
    block_len = VOCAB_SIZE // VP_BLOCKS
    hot_blocks = jax.random.permutation(key_hot, VP_BLOCKS)[:HOT_COUNT]
    hot_pick = jax.random.randint(key_pick, (BATCH_ROWS,), 0, HOT_COUNT)
    any_block = jax.random.randint(key_any, (BATCH_ROWS,), 0, VP_BLOCKS)
    use_hot = jax.random.randint(key_sel, (BATCH_ROWS,), 0, 4) < 3
    tok_block = jnp.where(use_hot, hot_blocks[hot_pick], any_block)
    tok_within = jax.random.randint(key_pos, (BATCH_ROWS,), 0, block_len)
    return (tok_block * block_len + tok_within).astype(jnp.int32)


def setup_inputs(seed: int = 0, part: int = 0) -> dict:
    shared_key, part_root = jax.random.split(jax.random.key(seed))
    part_key = jax.random.fold_in(part_root, part)
    key_hid, key_off, key_tok = jax.random.split(part_key, 3)
    key_tab, key_rowm, key_g1, key_b1, key_g2, key_b2 = jax.random.split(shared_key, 6)
    col_pos = jnp.arange(D, dtype=jnp.float32) / D
    hidden = jax.random.normal(key_hid, (BATCH_ROWS, D), jnp.float32) * (0.5 + 1.5 * col_pos)
    hidden = hidden + jax.random.normal(key_off, (BATCH_ROWS, 1), jnp.float32) * (1.0 + 2.0 * col_pos)
    tab_vals = jax.random.normal(key_tab, (VOCAB_SIZE, D), jnp.float32) * (0.5 + col_pos)
    tab_vals = (tab_vals + jax.random.normal(key_rowm, (VOCAB_SIZE, 1), jnp.float32)) * (D ** -0.5)
    return {
        "hidden": hidden.astype(jnp.bfloat16),
        "lnf_gain": 1.5 + 0.5 * jax.random.normal(key_g1, (D,), jnp.float32),
        "lnf_bias": 0.5 * jax.random.normal(key_b1, (D,), jnp.float32),
        "emb_table": tab_vals.astype(jnp.bfloat16),
        "next_tok": draw_tokens(key_tok),
        "eln_gain": 1.0 + 0.3 * jax.random.normal(key_g2, (D,), jnp.float32),
        "eln_bias": 0.5 * jax.random.normal(key_b2, (D,), jnp.float32),
    }


def layer_norm(rows_in, norm_gain, norm_bias):
    rows_f32 = rows_in.astype(jnp.float32)
    row_mean = jnp.mean(rows_f32, axis=-1, keepdims=True)
    row_var = jnp.mean(rows_f32 * rows_f32, axis=-1, keepdims=True) - row_mean * row_mean
    return (rows_f32 - row_mean) / jnp.sqrt(row_var + NORM_EPS) * norm_gain + norm_bias


def reference(hidden, lnf_gain, lnf_bias, emb_table, next_tok, eln_gain, eln_bias):
    normed = layer_norm(hidden, lnf_gain, lnf_bias).astype(jnp.bfloat16)
    logits = jnp.dot(normed, emb_table.T, preferred_element_type=jnp.float32)
    log_sum = jax.nn.logsumexp(logits, axis=-1)
    logprobs = logits - log_sum[:, None]
    tok_rows = jnp.take(emb_table, next_tok, axis=0)
    next_in = layer_norm(tok_rows, eln_gain, eln_bias).astype(jnp.bfloat16)
    return (logprobs, log_sum, next_in)
```

```python
import functools

import jax
import jax.numpy as jnp
from jax import lax
from jax.experimental import pallas as pl
from jax.experimental.pallas import tpu as pltpu
from jax.sharding import PartitionSpec as P

NORM_EPS = 1e-5
MESH = pl.DeviceIdType.MESH
F32 = jnp.float32
BF16 = jnp.bfloat16
LANES = 128


def cols_to_rows(cols):
    rows = cols[0].shape[0]
    lane = lax.broadcasted_iota(jnp.int32, (rows, LANES), 1)
    tile = jnp.zeros((rows, LANES), F32)
    for k, col in enumerate(cols):
        tile = jnp.where(lane == k, col, tile)
    full = jnp.concatenate([tile, jnp.zeros((LANES - rows, LANES), F32)], axis=0)
    return full.T[0:8, :]


def rows_to_cols(tile, rows):
    full = jnp.concatenate([tile, jnp.zeros((LANES - 8, LANES), F32)], axis=0)
    return full.T[0:rows, :]


def row_sums_tile(rows_f32):
    return cols_to_rows([
        jnp.sum(rows_f32, axis=1, keepdims=True),
        jnp.sum(rows_f32 * rows_f32, axis=1, keepdims=True),
    ])


def norm_rows(rows_f32, totals, gain, bias, full_width):
    mean = totals[0:1, :] / full_width
    var = totals[1:2, :] / full_width - mean * mean
    rstd = lax.rsqrt(var + NORM_EPS)
    pick = lax.broadcasted_iota(jnp.int32, (8, LANES), 0)
    both = jnp.where(pick == 0, mean, rstd)
    cols = rows_to_cols(both, rows_f32.shape[0])
    scaled = (rows_f32 - cols[:, 0:1]) * cols[:, 1:2]
    return (scaled * gain + bias).astype(BF16)


def logits_kernel(
    cfg, hid, gain, bias, tok, egain, ebias, tab,
    z, lse, nin,
    xn, out, xrecv, drecv, stg, tbuf, pick, ypick, runmax, runsum,
    ln_send, ln_recv, eln_send, eln_recv, fin_send, fin_recv,
    tab_sem, dsend_sem, drecv_sem, xsend_sem, xrecv_sem, ysend_sem, yrecv_sem,
    lns_sem, lnr_sem, els_sem, elr_sem, fis_sem, fir_sem,
):
    n, T, B, S, S2, n0, full_width = cfg
    rows = hid.shape[0]
    dp = lax.axis_index("dp")
    v = lax.axis_index("vp")
    t = lax.axis_index("tp")
    x = lax.div(t, 2)
    c = lax.rem(t, 2)

    def peer(d):
        pv = 1 - v if d >= 4 else v
        px = 1 - x if (d // 2) % 2 else x
        pc = 1 - c if d % 2 else c
        return (dp, pv, 2 * px + pc)

    def start_table(j):
        a = lax.div(j, n)
        i = j - a * n
        xx = (1 - x) + a * (2 * x - 1)
        for w in range(2):
            cc = 1 - c if w == 0 else c
            row = pl.multiple_of((2 * xx + cc) * B + i * T, LANES)
            slot = lax.rem(j, S)
            pltpu.make_async_copy(tab.at[pl.ds(row, T)], tbuf.at[slot, w], tab_sem.at[slot, w]).start()

    def wait_table(j, w):
        slot = lax.rem(j, S)
        pltpu.make_async_copy(tab.at[pl.ds(0, T)], tbuf.at[slot, w], tab_sem.at[slot, w]).wait()

    def first_row(j, w):
        a = lax.div(j, n)
        i = j - a * n
        xx = (1 - x) + a * (2 * x - 1)
        cc = 1 - c if w == 0 else c
        return v * (4 * B) + (2 * xx + cc) * B + i * T

    def d2d_copy(j):
        slot = lax.rem(j, S2)
        return pltpu.make_async_remote_copy(
            src_ref=stg.at[slot], dst_ref=drecv.at[j],
            send_sem=dsend_sem.at[slot], recv_sem=drecv_sem.at[j],
            device_id=peer(1), device_id_type=MESH)

    def x_copy(i):
        return pltpu.make_async_remote_copy(
            src_ref=out.at[i], dst_ref=xrecv.at[i],
            send_sem=xsend_sem.at[i], recv_sem=xrecv_sem.at[i],
            device_id=peer(2), device_id_type=MESH)

    def small_copy(src, dst, ssem, rsem, d):
        return pltpu.make_async_remote_copy(
            src_ref=src, dst_ref=dst.at[d], send_sem=ssem.at[d], recv_sem=rsem.at[d],
            device_id=peer(d), device_id_type=MESH)

    for j in range(S):
        start_table(j)

    barrier = pltpu.get_barrier_semaphore()
    for d in range(1, 8):
        pl.semaphore_signal(barrier, inc=1, device_id=peer(d), device_id_type=MESH)

    hid_f32 = hid[...].astype(F32)
    ln_send[...] = row_sums_tile(hid_f32)
    tok_cols = rows_to_cols(
        jnp.concatenate([tok[...].astype(F32), jnp.zeros((7, LANES), F32)], axis=0), rows)
    tok_col = tok_cols[:, 0:1].astype(jnp.int32)
    pick[...] = jnp.zeros_like(pick)
    runmax[...] = jnp.full(runmax.shape, -jnp.inf, F32)
    runsum[...] = jnp.zeros_like(runsum)
    pl.semaphore_wait(barrier, 7)

    for d in range(1, 4):
        small_copy(ln_send, ln_recv, lns_sem, lnr_sem, d).start()
    totals = ln_send[...]
    for d in range(1, 4):
        small_copy(ln_send, ln_recv, lns_sem, lnr_sem, d).wait()
        totals = totals + ln_recv[d]
    xn[...] = norm_rows(hid_f32, totals, gain[...], bias[...], full_width)

    def matmul(j, w):
        slot = lax.rem(j, S)
        return lax.dot_general(
            xn[...], tbuf[slot, w], (((1,), (1,)), ((), ())), preferred_element_type=F32)

    def pick_rows(j):
        slot = lax.rem(j, S)
        total = pick[...]
        for w in range(2):
            local = tok_col - first_row(j, w)
            hot = (lax.broadcasted_iota(jnp.int32, (rows, T), 1) == local).astype(F32).astype(BF16)
            total = total + jnp.dot(hot, tbuf[slot, w], preferred_element_type=F32)
        pick[...] = total

    def zcols(i):
        return pl.ds(pl.multiple_of(i * T, LANES), T)

    def send_half(j):
        wait_table(j, 0)

        @pl.when(j >= S2)
        def _():
            d2d_copy(j - S2).wait_send()

        stg[lax.rem(j, S2)] = matmul(j, 0)

    def combine_out(i):
        d2d_copy(i).wait_recv()
        out[i] = out[i] + drecv[i]

    def refill(j):
        @pl.when(j + S < 2 * n)
        def _():
            start_table(j + S)

    @pl.loop(0, n)
    def _(j):
        send_half(j)

        @pl.when(j >= 1)
        def _():
            combine_out(j - 1)

        d2d_copy(j).start()
        wait_table(j, 1)
        out[j] = matmul(j, 1)

        @pl.when(jnp.logical_and(j >= 1, j <= n0))
        def _():
            x_copy(j - 1).start()

        pick_rows(j)
        refill(j)

    @pl.loop(n, 2 * n)
    def _(j):
        send_half(j)

        @pl.when(j == n)
        def _():
            combine_out(n - 1)

        @pl.when(j > n)
        def _():
            d2d_copy(j - 1).wait_recv()
            z[:, zcols(j - 1 - n)] = z[:, zcols(j - 1 - n)] + drecv[j - 1]

        d2d_copy(j).start()
        wait_table(j, 1)
        z[:, zcols(j - n)] = matmul(j, 1)
        pick_rows(j)
        refill(j)

    d2d_copy(2 * n - 1).wait_recv()
    z[:, zcols(n - 1)] = z[:, zcols(n - 1)] + drecv[2 * n - 1]

    ycopy = pltpu.make_async_remote_copy(
        src_ref=pick, dst_ref=ypick, send_sem=ysend_sem, recv_sem=yrecv_sem,
        device_id=peer(4), device_id_type=MESH)
    ycopy.start()
    ycopy.wait()
    tok_rows = pick[...] + ypick[...]
    eln_send[...] = row_sums_tile(tok_rows)
    for d in range(1, 4):
        small_copy(eln_send, eln_recv, els_sem, elr_sem, d).start()
    for i in range(n0, n):
        x_copy(i).start()

    @pl.loop(0, n)
    def _(i):
        x_copy(i).wait_recv()
        m_old = runmax[...]
        m_new = m_old
        for k in range(T // LANES):
            cols = pl.ds(pl.multiple_of(i * T, LANES) + k * LANES, LANES)
            val = z[:, cols] + xrecv[i, :, k * LANES:(k + 1) * LANES]
            z[:, cols] = val
            m_new = jnp.maximum(m_new, val)
        s_new = runsum[...] * jnp.exp(m_old - m_new)
        for k in range(T // LANES):
            cols = pl.ds(pl.multiple_of(i * T, LANES) + k * LANES, LANES)
            s_new = s_new + jnp.exp(z[:, cols] - m_new)
        runmax[...] = m_new
        runsum[...] = s_new

    top = jnp.max(runmax[...], axis=1, keepdims=True)
    exp_sum = jnp.sum(runsum[...] * jnp.exp(runmax[...] - top), axis=1, keepdims=True)
    fin_send[...] = cols_to_rows([top, exp_sum])
    for d in range(1, 8):
        small_copy(fin_send, fin_recv, fis_sem, fir_sem, d).start()

    totals = eln_send[...]
    for d in range(1, 4):
        small_copy(eln_send, eln_recv, els_sem, elr_sem, d).wait()
        totals = totals + eln_recv[d]
    nin[...] = norm_rows(pick[...] + ypick[...], totals, egain[...], ebias[...], full_width)

    @pl.loop(0, n)
    def _(i):
        x_copy(i).wait_send()

    @pl.loop(2 * n - S2, 2 * n)
    def _(j):
        d2d_copy(j).wait_send()

    tiles = [fin_send[...]]
    for d in range(1, 8):
        small_copy(fin_send, fin_recv, fis_sem, fir_sem, d).wait()
        tiles.append(fin_recv[d])
    best = tiles[0][0:1, :]
    for tile in tiles[1:]:
        best = jnp.maximum(best, tile[0:1, :])
    total = jnp.zeros_like(best)
    for tile in tiles:
        total = total + tile[1:2, :] * jnp.exp(tile[0:1, :] - best)
    lse[...] = jnp.broadcast_to(best + jnp.log(total), lse.shape)


def finish_kernel(z, lse, nin, logp, log_sum, next_in, buf, sem):
    rows = z.shape[0]
    col = rows_to_cols(lse[...], rows)[:, 0:1]
    steps = rows // 8

    def put(b):
        return pltpu.make_async_copy(
            buf.at[pl.ds(8 * b, 8)], logp.at[pl.ds(8 * b, 8)], sem.at[b])

    for b in range(steps):
        buf[8 * b:8 * b + 8, :] = z[8 * b:8 * b + 8, :] - col[8 * b:8 * b + 8, :]
        if b >= 1:
            put(b - 1).start()
    next_in[...] = nin[...]
    log_sum[...] = lse[0:1, 0:rows]
    put(steps - 1).start()
    for b in range(steps):
        put(b).wait()


def solution(mesh):
    tp_size = mesh.shape["tp"]

    def per_device(hidden, lnf_gain, lnf_bias, emb_table, next_tok, eln_gain, eln_bias):
        rows, width = hidden.shape
        block = emb_table.shape[0] // tp_size
        T = 7 * LANES
        n = block // T
        S, S2, n0 = 3, 4, 25
        cfg = (n, T, block, S, S2, n0, float(width * tp_size))
        vmem = pl.BlockSpec(memory_space=pltpu.VMEM)
        hbm = pl.BlockSpec(memory_space=pl.ANY)
        tok_row = jnp.pad(next_tok.reshape(1, rows), ((0, 0), (0, LANES - rows)))
        dma = pltpu.SemaphoreType.DMA
        z, lse, nin = pl.pallas_call(
            functools.partial(logits_kernel, cfg),
            out_shape=(
                pltpu.VMEM((rows, block), F32),
                jax.ShapeDtypeStruct((8, LANES), F32),
                jax.ShapeDtypeStruct((rows, width), BF16),
            ),
            in_specs=[vmem] * 6 + [hbm],
            out_specs=(vmem, vmem, vmem),
            scratch_shapes=[
                pltpu.VMEM((rows, width), BF16),
                pltpu.VMEM((n, rows, T), F32),
                pltpu.VMEM((n, rows, T), F32),
                pltpu.VMEM((2 * n, rows, T), F32),
                pltpu.VMEM((S2, rows, T), F32),
                pltpu.VMEM((S, 2, T, width), BF16),
                pltpu.VMEM((rows, width), F32),
                pltpu.VMEM((rows, width), F32),
                pltpu.VMEM((rows, LANES), F32),
                pltpu.VMEM((rows, LANES), F32),
                pltpu.VMEM((8, LANES), F32),
                pltpu.VMEM((4, 8, LANES), F32),
                pltpu.VMEM((8, LANES), F32),
                pltpu.VMEM((4, 8, LANES), F32),
                pltpu.VMEM((8, LANES), F32),
                pltpu.VMEM((8, 8, LANES), F32),
                dma((S, 2)),
                dma((S2,)),
                dma((2 * n,)),
                dma((n,)),
                dma((n,)),
                dma,
                dma,
                dma((4,)),
                dma((4,)),
                dma((4,)),
                dma((4,)),
                dma((8,)),
                dma((8,)),
            ],
            compiler_params=pltpu.CompilerParams(
                collective_id=0, has_side_effects=True, vmem_limit_bytes=52 * 2**20),
        )(hidden, lnf_gain.reshape(1, width), lnf_bias.reshape(1, width), tok_row,
          eln_gain.reshape(1, width), eln_bias.reshape(1, width), emb_table)
        logp, log_sum, next_in = pl.pallas_call(
            finish_kernel,
            out_shape=(
                jax.ShapeDtypeStruct((rows, block), F32),
                jax.ShapeDtypeStruct((1, rows), F32),
                jax.ShapeDtypeStruct((rows, width), BF16),
            ),
            in_specs=[vmem, vmem, vmem],
            out_specs=(hbm, vmem, vmem),
            scratch_shapes=[pltpu.VMEM((rows, block), F32), dma((rows // 8,))],
            compiler_params=pltpu.CompilerParams(vmem_limit_bytes=20 * 2**20),
        )(z, lse, nin)
        return logp, log_sum.reshape(rows), next_in

    return jax.shard_map(
        per_device,
        mesh=mesh,
        in_specs=(P("dp", "tp"), P("tp"), P("tp"), P("vp", "tp"), P("dp"), P("tp"), P("tp")),
        out_specs=(P("dp", ("vp", "tp")), P("dp"), P("dp", "tp")),
        check_vma=False,
    )
```

```python
import functools

import jax
import jax.numpy as jnp
from jax import lax
from jax.experimental import pallas as pl
from jax.experimental.pallas import tpu as pltpu
from jax.sharding import PartitionSpec as P

NORM_EPS = 1e-5
MESH = pl.DeviceIdType.MESH
F32 = jnp.float32
BF16 = jnp.bfloat16
LANES = 128


def diagonal(rows):
    return (lax.broadcasted_iota(jnp.int32, (rows, LANES), 0)
            == lax.broadcasted_iota(jnp.int32, (rows, LANES), 1))


def col_to_row(col):
    return jnp.sum(jnp.where(diagonal(col.shape[0]), col, jnp.zeros_like(col)), axis=0, keepdims=True)


def row_to_col(row, rows):
    return jnp.sum(jnp.where(diagonal(rows), row, jnp.zeros_like(row)), axis=1, keepdims=True)


def two_rows(first, second):
    sub = lax.broadcasted_iota(jnp.int32, (8, LANES), 0)
    return jnp.where(sub == 0, first, second)


def row_sums_tile(rows_f32):
    return two_rows(
        col_to_row(jnp.sum(rows_f32, axis=1, keepdims=True)),
        col_to_row(jnp.sum(rows_f32 * rows_f32, axis=1, keepdims=True)))


def norm_rows(rows_f32, totals, gain, bias, full_width):
    rows = rows_f32.shape[0]
    mean = totals[0:1, :] / full_width
    var = totals[1:2, :] / full_width - mean * mean
    rstd = lax.rsqrt(var + NORM_EPS)
    scaled = (rows_f32 - row_to_col(mean, rows)) * row_to_col(rstd, rows)
    return (scaled * gain + bias).astype(BF16)


def logits_kernel(
    cfg, hid_hbm, gain_hbm, bias_hbm, tok_hbm, egain_hbm, ebias_hbm, tab,
    z, lse, nin,
    hid, gain, bias, tok, egain, ebias, in_sem,
    hds_sem, hdr_sem, hxs_sem, hxr_sem,
    xn, out, xrecv, drecv, stg, tbuf, pick, ypick, runmax, runsum,
    ln_send, ln_recv, eln_send, eln_recv, fin_send, fin_recv,
    tab_sem, dsend_sem, drecv_sem, xsend_sem, xrecv_sem, ysend_sem, yrecv_sem,
    lns_sem, lnr_sem, els_sem, elr_sem, fis_sem, fir_sem,
):
    n, T, B, S, S2, n0, full_width, head = cfg
    rows = hid.shape[0]
    dp = lax.axis_index("dp")
    v = lax.axis_index("vp")
    t = lax.axis_index("tp")
    x = lax.div(t, 2)
    c = lax.rem(t, 2)

    def peer(d):
        pv = 1 - v if d >= 4 else v
        px = 1 - x if (d // 2) % 2 else x
        pc = 1 - c if d % 2 else c
        return (dp, pv, 2 * px + pc)

    def start_table(j):
        a = lax.div(j, n)
        i = j - a * n
        xx = (1 - x) + a * (2 * x - 1)
        for w in range(2):
            cc = 1 - c if w == 0 else c
            row = pl.multiple_of((2 * xx + cc) * B + i * T, LANES)
            slot = lax.rem(j, S)
            pltpu.make_async_copy(tab.at[pl.ds(row, T)], tbuf.at[slot, w], tab_sem.at[slot, w]).start()

    def wait_table(j, w):
        slot = lax.rem(j, S)
        pltpu.make_async_copy(tab.at[pl.ds(0, T)], tbuf.at[slot, w], tab_sem.at[slot, w]).wait()

    def first_row(j, w):
        a = lax.div(j, n)
        i = j - a * n
        xx = (1 - x) + a * (2 * x - 1)
        cc = 1 - c if w == 0 else c
        return v * (4 * B) + (2 * xx + cc) * B + i * T

    def d2d_copy(j):
        slot = lax.rem(j, S2)
        return pltpu.make_async_remote_copy(
            src_ref=stg.at[slot], dst_ref=drecv.at[j],
            send_sem=dsend_sem.at[slot], recv_sem=drecv_sem.at[j],
            device_id=peer(1), device_id_type=MESH)

    def x_copy(i):
        return pltpu.make_async_remote_copy(
            src_ref=out.at[i], dst_ref=xrecv.at[i],
            send_sem=xsend_sem.at[i], recv_sem=xrecv_sem.at[i],
            device_id=peer(2), device_id_type=MESH)

    def small_copy(src, dst, ssem, rsem, d):
        return pltpu.make_async_remote_copy(
            src_ref=src, dst_ref=dst.at[d], send_sem=ssem.at[d], recv_sem=rsem.at[d],
            device_id=peer(d), device_id_type=MESH)

    barrier = pltpu.get_barrier_semaphore()
    for d in (6, 7, 5, 4, 2, 3, 1):
        pl.semaphore_signal(barrier, inc=1, device_id=peer(d), device_id_type=MESH)

    pairs = ((hid_hbm, hid), (gain_hbm, gain), (bias_hbm, bias), (tok_hbm, tok),
             (egain_hbm, egain), (ebias_hbm, ebias))
    loads = [pltpu.make_async_copy(src, dst, in_sem.at[k]) for k, (src, dst) in enumerate(pairs)]
    for load in loads:
        load.start()
    for j in range(S):
        start_table(j)

    loads[0].wait()
    hid_f32 = hid[...].astype(F32)
    ln_send[...] = row_sums_tile(hid_f32)
    pl.semaphore_wait(barrier, 7)

    for d in range(1, 4):
        small_copy(ln_send, ln_recv, lns_sem, lnr_sem, d).start()
    for load in loads[1:]:
        load.wait()
    eye = (lax.broadcasted_iota(jnp.int32, (rows, rows), 0)
           == lax.broadcasted_iota(jnp.int32, (rows, rows), 1))
    tok_col = jnp.sum(
        jnp.where(eye, tok[...].astype(F32), 0.0), axis=1, keepdims=True).astype(jnp.int32)
    pick[...] = jnp.zeros_like(pick)
    runmax[...] = jnp.full(runmax.shape, -jnp.inf, F32)
    runsum[...] = jnp.zeros_like(runsum)
    wait_table(0, 0)
    wait_table(0, 1)
    totals = ln_send[...]
    for d in range(1, 4):
        small_copy(ln_send, ln_recv, lns_sem, lnr_sem, d).wait()
        totals = totals + ln_recv[d]
    xn[...] = norm_rows(hid_f32, totals, gain[...], bias[...], full_width)

    def matmul(j, w):
        slot = lax.rem(j, S)
        return lax.dot_general(
            xn[...], tbuf[slot, w], (((1,), (1,)), ((), ())), preferred_element_type=F32)

    def pick_rows(j):
        slot = lax.rem(j, S)
        total = pick[...]
        for w in range(2):
            local = tok_col - first_row(j, w)
            hot = (lax.broadcasted_iota(jnp.int32, (rows, T), 1) == local).astype(F32).astype(BF16)
            total = total + jnp.dot(hot, tbuf[slot, w], preferred_element_type=F32)
        pick[...] = total

    def zcols(i):
        return pl.ds(pl.multiple_of(i * T, LANES), T)

    def send_half(j):
        wait_table(j, 0)

        @pl.when(j > S2)
        def _():
            d2d_copy(j - S2).wait_send()

        stg[lax.rem(j, S2)] = matmul(j, 0)

    def combine_out(i):
        d2d_copy(i).wait_recv()
        out[i] = out[i] + drecv[i]

    def refill(j):
        @pl.when(j + S < 2 * n)
        def _():
            start_table(j + S)

    def head_d2d(k):
        cols = pl.ds(head[k], head[k + 1] - head[k])
        return pltpu.make_async_remote_copy(
            src_ref=stg.at[0, :, cols], dst_ref=drecv.at[0, :, cols],
            send_sem=hds_sem.at[k], recv_sem=hdr_sem.at[k],
            device_id=peer(1), device_id_type=MESH)

    def head_x(k):
        cols = pl.ds(head[k], head[k + 1] - head[k])
        return pltpu.make_async_remote_copy(
            src_ref=out.at[0, :, cols], dst_ref=xrecv.at[0, :, cols],
            send_sem=hxs_sem.at[k], recv_sem=hxr_sem.at[k],
            device_id=peer(2), device_id_type=MESH)

    def head_matmul(k, w):
        return lax.dot_general(
            xn[...], tbuf[0, w, head[k]:head[k + 1], :], (((1,), (1,)), ((), ())),
            preferred_element_type=F32)

    def head_combine(k):
        head_d2d(k).wait_recv()
        cols = slice(head[k], head[k + 1])
        out[0, :, cols] = out[0, :, cols] + drecv[0, :, cols]

    pieces = len(head) - 1
    for k in range(pieces):
        stg[0, :, head[k]:head[k + 1]] = head_matmul(k, 0)
        out[0, :, head[k]:head[k + 1]] = head_matmul(k, 1)
        head_d2d(k).start()
        if k >= 1:
            head_combine(k - 1)
            head_x(k - 1).start()
    pick_rows(0)
    refill(0)
    head_combine(pieces - 1)
    for k in range(pieces):
        head_d2d(k).wait_send()
    head_x(pieces - 1).start()

    @pl.loop(1, n)
    def _(j):
        send_half(j)

        @pl.when(j >= 2)
        def _():
            combine_out(j - 1)

        d2d_copy(j).start()
        wait_table(j, 1)
        out[j] = matmul(j, 1)

        @pl.when(jnp.logical_and(j >= 2, j <= n0))
        def _():
            x_copy(j - 1).start()

        pick_rows(j)
        refill(j)

    @pl.loop(n, 2 * n)
    def _(j):
        send_half(j)

        @pl.when(j == n)
        def _():
            combine_out(n - 1)

        @pl.when(j > n)
        def _():
            d2d_copy(j - 1).wait_recv()
            z[:, zcols(j - 1 - n)] = z[:, zcols(j - 1 - n)] + drecv[j - 1]

        d2d_copy(j).start()
        wait_table(j, 1)
        z[:, zcols(j - n)] = matmul(j, 1)
        pick_rows(j)
        refill(j)

    d2d_copy(2 * n - 1).wait_recv()
    z[:, zcols(n - 1)] = z[:, zcols(n - 1)] + drecv[2 * n - 1]

    ycopy = pltpu.make_async_remote_copy(
        src_ref=pick, dst_ref=ypick, send_sem=ysend_sem, recv_sem=yrecv_sem,
        device_id=peer(4), device_id_type=MESH)
    ycopy.start()
    ycopy.wait()
    tok_rows = pick[...] + ypick[...]
    eln_send[...] = row_sums_tile(tok_rows)
    for d in range(1, 4):
        small_copy(eln_send, eln_recv, els_sem, elr_sem, d).start()
    for i in range(n0, n):
        x_copy(i).start()

    def absorb(i):
        m_old = runmax[...]
        m_new = m_old
        for k in range(T // LANES):
            cols = pl.ds(pl.multiple_of(i * T, LANES) + k * LANES, LANES)
            val = z[:, cols] + xrecv[i, :, k * LANES:(k + 1) * LANES]
            z[:, cols] = val
            m_new = jnp.maximum(m_new, val)
        s_new = runsum[...] * jnp.exp(m_old - m_new)
        for k in range(T // LANES):
            cols = pl.ds(pl.multiple_of(i * T, LANES) + k * LANES, LANES)
            s_new = s_new + jnp.exp(z[:, cols] - m_new)
        runmax[...] = m_new
        runsum[...] = s_new

    for k in range(pieces):
        head_x(k).wait_recv()

    @pl.loop(0, n)
    def _(i):
        @pl.when(i >= 1)
        def _():
            x_copy(i).wait_recv()

        absorb(i)

    top = jnp.max(runmax[...], axis=1, keepdims=True)
    exp_sum = jnp.sum(runsum[...] * jnp.exp(runmax[...] - top), axis=1, keepdims=True)
    fin_send[...] = two_rows(col_to_row(top), col_to_row(exp_sum))
    for d in (6, 7, 5, 4, 2, 3, 1):
        small_copy(fin_send, fin_recv, fis_sem, fir_sem, d).start()

    totals = eln_send[...]
    for d in range(1, 4):
        small_copy(eln_send, eln_recv, els_sem, elr_sem, d).wait()
        totals = totals + eln_recv[d]
    nin[...] = norm_rows(pick[...] + ypick[...], totals, egain[...], ebias[...], full_width)

    for k in range(pieces):
        head_x(k).wait_send()

    @pl.loop(1, n)
    def _(i):
        x_copy(i).wait_send()

    @pl.loop(2 * n - S2, 2 * n)
    def _(j):
        d2d_copy(j).wait_send()

    tiles = [fin_send[...]]
    for d in range(1, 8):
        small_copy(fin_send, fin_recv, fis_sem, fir_sem, d).wait()
        tiles.append(fin_recv[d])
    best = tiles[0][0:1, :]
    for tile in tiles[1:]:
        best = jnp.maximum(best, tile[0:1, :])
    total = jnp.zeros_like(best)
    for tile in tiles:
        total = total + tile[1:2, :] * jnp.exp(tile[0:1, :] - best)
    lse[...] = jnp.broadcast_to(best + jnp.log(total), lse.shape)


def finish_kernel(z, lse, nin, logp, log_sum, next_in, buf, row, sem, small_sem):
    rows = z.shape[0]
    col = row_to_col(lse[0:1, :], rows)
    steps = rows // 8

    def put(b):
        return pltpu.make_async_copy(
            buf.at[pl.ds(8 * b, 8)], logp.at[pl.ds(8 * b, 8)], sem.at[b])

    row[...] = lse[0:1, 0:rows]
    nin_copy = pltpu.make_async_copy(nin, next_in, small_sem.at[0])
    nin_copy.start()
    for b in range(steps):
        buf[8 * b:8 * b + 8, :] = z[8 * b:8 * b + 8, :] - col[8 * b:8 * b + 8, :]
        if b >= 1:
            put(b - 1).start()
    put(steps - 1).start()
    row_copy = pltpu.make_async_copy(row, log_sum, small_sem.at[1])
    row_copy.start()
    nin_copy.wait()
    row_copy.wait()
    for b in range(steps):
        put(b).wait()


def solution(mesh):
    tp_size = mesh.shape["tp"]

    def per_device(hidden, lnf_gain, lnf_bias, emb_table, next_tok, eln_gain, eln_bias):
        rows, width = hidden.shape
        block = emb_table.shape[0] // tp_size
        T = 7 * LANES
        n = block // T
        S, S2, n0 = 3, 4, 25
        head = (0, LANES, 3 * LANES, T)
        cfg = (n, T, block, S, S2, n0, float(width * tp_size), head)
        vmem = pl.BlockSpec(memory_space=pltpu.VMEM)
        hbm = pl.BlockSpec(memory_space=pl.ANY)
        dma = pltpu.SemaphoreType.DMA
        z, lse, nin = pl.pallas_call(
            functools.partial(logits_kernel, cfg),
            out_shape=(
                pltpu.VMEM((rows, block), F32),
                pltpu.VMEM((8, LANES), F32),
                pltpu.VMEM((rows, width), BF16),
            ),
            in_specs=[hbm] * 7,
            out_specs=(vmem, vmem, vmem),
            scratch_shapes=[
                pltpu.VMEM((rows, width), BF16),
                pltpu.VMEM((1, width), F32),
                pltpu.VMEM((1, width), F32),
                pltpu.VMEM((1, rows), jnp.int32),
                pltpu.VMEM((1, width), F32),
                pltpu.VMEM((1, width), F32),
                dma((6,)),
                dma((3,)),
                dma((3,)),
                dma((3,)),
                dma((3,)),
                pltpu.VMEM((rows, width), BF16),
                pltpu.VMEM((n, rows, T), F32),
                pltpu.VMEM((n, rows, T), F32),
                pltpu.VMEM((2 * n, rows, T), F32),
                pltpu.VMEM((S2, rows, T), F32),
                pltpu.VMEM((S, 2, T, width), BF16),
                pltpu.VMEM((rows, width), F32),
                pltpu.VMEM((rows, width), F32),
                pltpu.VMEM((rows, LANES), F32),
                pltpu.VMEM((rows, LANES), F32),
                pltpu.VMEM((8, LANES), F32),
                pltpu.VMEM((4, 8, LANES), F32),
                pltpu.VMEM((8, LANES), F32),
                pltpu.VMEM((4, 8, LANES), F32),
                pltpu.VMEM((8, LANES), F32),
                pltpu.VMEM((8, 8, LANES), F32),
                dma((S, 2)),
                dma((S2,)),
                dma((2 * n,)),
                dma((n,)),
                dma((n,)),
                dma,
                dma,
                dma((4,)),
                dma((4,)),
                dma((4,)),
                dma((4,)),
                dma((8,)),
                dma((8,)),
            ],
            compiler_params=pltpu.CompilerParams(
                collective_id=0, has_side_effects=True, vmem_limit_bytes=52 * 2**20),
        )(hidden, lnf_gain.reshape(1, width), lnf_bias.reshape(1, width), next_tok.reshape(1, rows),
          eln_gain.reshape(1, width), eln_bias.reshape(1, width), emb_table)
        logp, log_sum, next_in = pl.pallas_call(
            finish_kernel,
            out_shape=(
                jax.ShapeDtypeStruct((rows, block), F32),
                jax.ShapeDtypeStruct((1, rows), F32),
                jax.ShapeDtypeStruct((rows, width), BF16),
            ),
            in_specs=[vmem, vmem, vmem],
            out_specs=(hbm, hbm, hbm),
            scratch_shapes=[
                pltpu.VMEM((rows, block), F32), pltpu.VMEM((1, rows), F32), dma((rows // 8,)), dma((2,))],
            compiler_params=pltpu.CompilerParams(vmem_limit_bytes=20 * 2**20),
        )(z, lse, nin)
        return logp, log_sum.reshape(rows), next_in

    return jax.shard_map(
        per_device,
        mesh=mesh,
        in_specs=(P("dp", "tp"), P("tp"), P("tp"), P("vp", "tp"), P("dp"), P("tp"), P("tp")),
        out_specs=(P("dp", ("vp", "tp")), P("dp"), P("dp", "tp")),
        check_vma=False,
    )
```

```python
import functools

import jax
import jax.numpy as jnp
from jax import lax
from jax.experimental import pallas as pl
from jax.experimental.pallas import tpu as pltpu
from jax.sharding import PartitionSpec as P

NORM_EPS = 1e-5
MESH = pl.DeviceIdType.MESH
F32 = jnp.float32
BF16 = jnp.bfloat16
LANES = 128


def diagonal(rows):
    return (lax.broadcasted_iota(jnp.int32, (rows, LANES), 0)
            == lax.broadcasted_iota(jnp.int32, (rows, LANES), 1))


def col_to_row(col):
    return jnp.sum(jnp.where(diagonal(col.shape[0]), col, jnp.zeros_like(col)), axis=0, keepdims=True)


def row_to_col(row, rows):
    return jnp.sum(jnp.where(diagonal(rows), row, jnp.zeros_like(row)), axis=1, keepdims=True)


def two_rows(first, second):
    sub = lax.broadcasted_iota(jnp.int32, (8, LANES), 0)
    return jnp.where(sub == 0, first, second)


def row_sums_tile(rows_f32):
    return two_rows(
        col_to_row(jnp.sum(rows_f32, axis=1, keepdims=True)),
        col_to_row(jnp.sum(rows_f32 * rows_f32, axis=1, keepdims=True)))


def norm_rows(rows_f32, totals, gain, bias, full_width):
    rows = rows_f32.shape[0]
    mean = totals[0:1, :] / full_width
    var = totals[1:2, :] / full_width - mean * mean
    rstd = lax.rsqrt(var + NORM_EPS)
    scaled = (rows_f32 - row_to_col(mean, rows)) * row_to_col(rstd, rows)
    return (scaled * gain + bias).astype(BF16)


def logits_kernel(
    cfg, hid_hbm, gain_hbm, bias_hbm, tok_hbm, egain_hbm, ebias_hbm, tab,
    z, lse, nin,
    hid, gain, bias, tok, egain, ebias, in_sem,
    hds_sem, hdr_sem, hxr_sem,
    xn, out, xrecv, drecv, stg, tbuf, pick, ypick, runmax, runsum,
    ln_send, ln_recv, eln_send, eln_recv, fin_send, fin_recv,
    tab_sem, dsend_sem, drecv_sem, xsend_sem, xrecv_sem, ysend_sem, yrecv_sem,
    lns_sem, lnr_sem, els_sem, elr_sem, fis_sem, fir_sem,
):
    n, T, B, S, S2, n0, full_width, head, groups = cfg
    rows = hid.shape[0]
    dp = lax.axis_index("dp")
    v = lax.axis_index("vp")
    t = lax.axis_index("tp")
    x = lax.div(t, 2)
    c = lax.rem(t, 2)

    def peer(d):
        pv = 1 - v if d >= 4 else v
        px = 1 - x if (d // 2) % 2 else x
        pc = 1 - c if d % 2 else c
        return (dp, pv, 2 * px + pc)

    def start_table(j):
        a = lax.div(j, n)
        i = j - a * n
        xx = (1 - x) + a * (2 * x - 1)
        for w in range(2):
            cc = 1 - c if w == 0 else c
            row = pl.multiple_of((2 * xx + cc) * B + i * T, LANES)
            slot = lax.rem(j, S)
            pltpu.make_async_copy(tab.at[pl.ds(row, T)], tbuf.at[slot, w], tab_sem.at[slot]).start()

    def wait_table(j):
        slot = lax.rem(j, S)
        pltpu.make_async_copy(tbuf.at[slot], tbuf.at[slot], tab_sem.at[slot]).wait()

    def first_row(j, w):
        a = lax.div(j, n)
        i = j - a * n
        xx = (1 - x) + a * (2 * x - 1)
        cc = 1 - c if w == 0 else c
        return v * (4 * B) + (2 * xx + cc) * B + i * T

    def d2d_copy(j):
        slot = lax.rem(j, S2)
        return pltpu.make_async_remote_copy(
            src_ref=stg.at[slot], dst_ref=drecv.at[slot],
            send_sem=dsend_sem.at[slot], recv_sem=drecv_sem.at[slot],
            device_id=peer(1), device_id_type=MESH)

    def x_copy(g):
        first, last = groups[g]
        part = pl.ds(first, last - first)
        return pltpu.make_async_remote_copy(
            src_ref=out.at[part], dst_ref=xrecv.at[part],
            send_sem=xsend_sem, recv_sem=xrecv_sem.at[g],
            device_id=peer(2), device_id_type=MESH)

    def small_copy(src, dst, ssem, rsem, d):
        return pltpu.make_async_remote_copy(
            src_ref=src, dst_ref=dst.at[d - 1], send_sem=ssem, recv_sem=rsem,
            device_id=peer(d), device_id_type=MESH)

    def wait_small(dst, ssem, rsem):
        both = pltpu.make_async_remote_copy(
            src_ref=dst, dst_ref=dst, send_sem=ssem, recv_sem=rsem,
            device_id=peer(1), device_id_type=MESH)
        both.wait_recv()
        both.wait_send()

    barrier = pltpu.get_barrier_semaphore()
    for d in (4, 2, 3, 1):
        pl.semaphore_signal(barrier, inc=1, device_id=peer(d), device_id_type=MESH)

    pairs = ((hid_hbm, hid), (gain_hbm, gain), (bias_hbm, bias), (tok_hbm, tok),
             (egain_hbm, egain), (ebias_hbm, ebias))
    loads = [pltpu.make_async_copy(src, dst, in_sem.at[k]) for k, (src, dst) in enumerate(pairs)]
    for load in loads:
        load.start()
    for j in range(S):
        start_table(j)

    loads[0].wait()
    hid_f32 = hid[...].astype(F32)
    ln_send[...] = row_sums_tile(hid_f32)
    pl.semaphore_wait(barrier, 4)

    for d in (2, 3, 1):
        small_copy(ln_send, ln_recv, lns_sem, lnr_sem, d).start()
    for load in loads[1:]:
        load.wait()
    eye = (lax.broadcasted_iota(jnp.int32, (rows, rows), 0)
           == lax.broadcasted_iota(jnp.int32, (rows, rows), 1))
    tok_col = jnp.sum(
        jnp.where(eye, tok[...].astype(F32), 0.0), axis=1, keepdims=True).astype(jnp.int32)
    pick[...] = jnp.zeros_like(pick)
    runmax[...] = jnp.full(runmax.shape, -jnp.inf, F32)
    runsum[...] = jnp.zeros_like(runsum)
    wait_table(0)
    totals = ln_send[...]
    wait_small(ln_recv, lns_sem, lnr_sem)
    for d in range(3):
        totals = totals + ln_recv[d]
    xn[...] = norm_rows(hid_f32, totals, gain[...], bias[...], full_width)

    def matmul(j, w):
        slot = lax.rem(j, S)
        return lax.dot_general(
            xn[...], tbuf[slot, w], (((1,), (1,)), ((), ())), preferred_element_type=F32)

    def pick_rows(j):
        slot = lax.rem(j, S)
        total = pick[...]
        for w in range(2):
            local = tok_col - first_row(j, w)
            hot = (lax.broadcasted_iota(jnp.int32, (rows, T), 1) == local).astype(F32).astype(BF16)
            total = total + jnp.dot(hot, tbuf[slot, w], preferred_element_type=F32)
        pick[...] = total

    def zcols(i):
        return pl.ds(pl.multiple_of(i * T, LANES), T)

    def send_half(j):
        wait_table(j)

        @pl.when(j > S2)
        def _():
            d2d_copy(j - S2).wait_send()

        stg[lax.rem(j, S2)] = matmul(j, 0)

    def combine_out(i):
        d2d_copy(i).wait_recv()
        out[i] = out[i] + drecv[lax.rem(i, S2)]

    def refill(j):
        @pl.when(j + S < 2 * n)
        def _():
            start_table(j + S)

    def head_d2d(k):
        cols = pl.ds(head[k], head[k + 1] - head[k])
        return pltpu.make_async_remote_copy(
            src_ref=stg.at[0, :, cols], dst_ref=drecv.at[0, :, cols],
            send_sem=hds_sem.at[k], recv_sem=hdr_sem.at[k],
            device_id=peer(1), device_id_type=MESH)

    def head_x(k):
        cols = pl.ds(head[k], head[k + 1] - head[k])
        return pltpu.make_async_remote_copy(
            src_ref=out.at[0, :, cols], dst_ref=xrecv.at[0, :, cols],
            send_sem=xsend_sem, recv_sem=hxr_sem,
            device_id=peer(2), device_id_type=MESH)

    def head_matmul(k, w):
        return lax.dot_general(
            xn[...], tbuf[0, w, head[k]:head[k + 1], :], (((1,), (1,)), ((), ())),
            preferred_element_type=F32)

    def head_combine(k):
        head_d2d(k).wait_recv()
        cols = slice(head[k], head[k + 1])
        out[0, :, cols] = out[0, :, cols] + drecv[0, :, cols]

    pieces = len(head) - 1

    def head_give(k):
        stg[0, :, head[k]:head[k + 1]] = head_matmul(k, 0)

    def head_keep(k):
        out[0, :, head[k]:head[k + 1]] = head_matmul(k, 1)

    @pl.when(c == 0)
    def _():
        for k in range(pieces):
            head_keep(k)
        for k in range(pieces):
            head_give(k)
            head_combine(k)
            head_d2d(k).start()
            if k >= 1:
                head_x(k - 1).start()
        pick_rows(0)
        head_x(pieces - 1).start()

    @pl.when(c == 1)
    def _():
        head_give(0)
        for k in range(pieces):
            if k + 1 < pieces:
                head_give(k + 1)
            else:
                head_keep(0)
            head_d2d(k).start()
        for k in range(1, pieces):
            head_keep(k)
            head_combine(k - 1)
            if k >= 2:
                head_x(k - 2).start()
        head_x(pieces - 2).start()
        pick_rows(0)
        head_combine(pieces - 1)
        head_x(pieces - 1).start()

    refill(0)
    for k in range(pieces):
        head_d2d(k).wait_send()

    @pl.loop(1, n)
    def _(j):
        send_half(j)

        @pl.when(j >= 2)
        def _():
            combine_out(j - 1)

        d2d_copy(j).start()
        out[j] = matmul(j, 1)

        for g in range(n0):
            @pl.when(j == groups[g][1])
            def _():
                x_copy(g).start()

        pick_rows(j)
        refill(j)

    @pl.loop(n, 2 * n)
    def _(j):
        send_half(j)

        @pl.when(j == n)
        def _():
            combine_out(n - 1)

        @pl.when(j > n)
        def _():
            d2d_copy(j - 1).wait_recv()
            z[:, zcols(j - 1 - n)] = z[:, zcols(j - 1 - n)] + drecv[lax.rem(j - 1, S2)]

        d2d_copy(j).start()
        z[:, zcols(j - n)] = matmul(j, 1)
        pick_rows(j)
        refill(j)

    d2d_copy(2 * n - 1).wait_recv()
    z[:, zcols(n - 1)] = z[:, zcols(n - 1)] + drecv[(2 * n - 1) % S2]

    ycopy = pltpu.make_async_remote_copy(
        src_ref=pick, dst_ref=ypick, send_sem=ysend_sem, recv_sem=yrecv_sem,
        device_id=peer(4), device_id_type=MESH)
    ycopy.start()
    ycopy.wait()
    tok_rows = pick[...] + ypick[...]
    eln_send[...] = row_sums_tile(tok_rows)
    for d in range(1, 4):
        small_copy(eln_send, eln_recv, els_sem, elr_sem, d).start()
    for g in range(n0, len(groups)):
        x_copy(g).start()

    def absorb(i):
        m_old = runmax[...]
        m_new = m_old
        for k in range(T // LANES):
            cols = pl.ds(pl.multiple_of(i * T, LANES) + k * LANES, LANES)
            val = z[:, cols] + xrecv[i, :, k * LANES:(k + 1) * LANES]
            z[:, cols] = val
            m_new = jnp.maximum(m_new, val)
        s_new = runsum[...] * jnp.exp(m_old - m_new)
        for k in range(T // LANES):
            cols = pl.ds(pl.multiple_of(i * T, LANES) + k * LANES, LANES)
            s_new = s_new + jnp.exp(z[:, cols] - m_new)
        runmax[...] = m_new
        runsum[...] = s_new

    pltpu.make_async_remote_copy(
        src_ref=out.at[0], dst_ref=xrecv.at[0], send_sem=xsend_sem, recv_sem=hxr_sem,
        device_id=peer(2), device_id_type=MESH).wait_recv()

    absorb(0)
    for g, (first, last) in enumerate(groups):
        x_copy(g).wait_recv()

        @pl.loop(first, last)
        def _(i):
            absorb(i)

    top = jnp.max(runmax[...], axis=1, keepdims=True)
    exp_sum = jnp.sum(runsum[...] * jnp.exp(runmax[...] - top), axis=1, keepdims=True)
    fin_send[...] = two_rows(col_to_row(top), col_to_row(exp_sum))
    for d in (6, 7, 5, 4, 2, 3, 1):
        small_copy(fin_send, fin_recv, fis_sem, fir_sem, d).start()

    totals = eln_send[...]
    wait_small(eln_recv, els_sem, elr_sem)
    for d in range(3):
        totals = totals + eln_recv[d]
    nin[...] = norm_rows(pick[...] + ypick[...], totals, egain[...], ebias[...], full_width)

    pltpu.make_async_remote_copy(
        src_ref=out, dst_ref=xrecv, send_sem=xsend_sem, recv_sem=hxr_sem,
        device_id=peer(2), device_id_type=MESH).wait_send()

    @pl.loop(2 * n - S2, 2 * n)
    def _(j):
        d2d_copy(j).wait_send()

    tiles = [fin_send[...]]
    wait_small(fin_recv, fis_sem, fir_sem)
    for d in range(7):
        tiles.append(fin_recv[d])
    best = tiles[0][0:1, :]
    for tile in tiles[1:]:
        best = jnp.maximum(best, tile[0:1, :])
    total = jnp.zeros_like(best)
    for tile in tiles:
        total = total + tile[1:2, :] * jnp.exp(tile[0:1, :] - best)
    lse[...] = jnp.broadcast_to(best + jnp.log(total), lse.shape)


def finish_kernel(z, lse, nin, logp, log_sum, next_in, buf, row, sem, small_sem):
    rows, width = z.shape
    col = row_to_col(lse[0:1, :], rows)
    cuts = [0, 16 * LANES, 48 * LANES, 112 * LANES, width]
    parts = [(0, lo, hi) for lo, hi in zip(cuts, cuts[1:])]
    parts += [(r, 0, width) for r in range(8, rows, 8)]

    def put(b):
        r, lo, hi = parts[b]
        part = (pl.ds(r, 8), pl.ds(lo, hi - lo))
        return pltpu.make_async_copy(buf.at[part], logp.at[part], sem)

    row[...] = lse[0:1, 0:rows]
    nin_copy = pltpu.make_async_copy(nin, next_in, small_sem.at[0])
    row_copy = pltpu.make_async_copy(row, log_sum, small_sem.at[1])
    for b, (r, lo, hi) in enumerate(parts):
        buf[r:r + 8, lo:hi] = z[r:r + 8, lo:hi] - col[r:r + 8, :]
        if b >= 1:
            put(b - 1).start()
        if b == 3:
            nin_copy.start()
            row_copy.start()
    put(len(parts) - 1).start()
    nin_copy.wait()
    row_copy.wait()
    pltpu.make_async_copy(buf, logp, sem).wait()


def solution(mesh):
    tp_size = mesh.shape["tp"]

    def per_device(hidden, lnf_gain, lnf_bias, emb_table, next_tok, eln_gain, eln_bias):
        rows, width = hidden.shape
        block = emb_table.shape[0] // tp_size
        T = 7 * LANES
        n = block // T
        S, S2, n0 = 3, 4, 8
        sizes = (1, 1, 2, 5, 5, 5, 5, 5, 2, 2, 1)
        groups, at = [], 1
        for size in sizes:
            groups.append((at, at + size))
            at += size
        head = (0, LANES, 3 * LANES, T)
        cfg = (n, T, block, S, S2, n0, float(width * tp_size), head, tuple(groups))
        vmem = pl.BlockSpec(memory_space=pltpu.VMEM)
        hbm = pl.BlockSpec(memory_space=pl.ANY)
        dma = pltpu.SemaphoreType.DMA
        z, lse, nin = pl.pallas_call(
            functools.partial(logits_kernel, cfg),
            out_shape=(
                pltpu.VMEM((rows, block), F32),
                pltpu.VMEM((8, LANES), F32),
                pltpu.VMEM((rows, width), BF16),
            ),
            in_specs=[hbm] * 7,
            out_specs=(vmem, vmem, vmem),
            scratch_shapes=[
                pltpu.VMEM((rows, width), BF16),
                pltpu.VMEM((1, width), F32),
                pltpu.VMEM((1, width), F32),
                pltpu.VMEM((1, rows), jnp.int32),
                pltpu.VMEM((1, width), F32),
                pltpu.VMEM((1, width), F32),
                dma((6,)),
                dma((3,)),
                dma((3,)),
                dma,
                pltpu.VMEM((rows, width), BF16),
                pltpu.VMEM((n, rows, T), F32),
                pltpu.VMEM((n, rows, T), F32),
                pltpu.VMEM((S2, rows, T), F32),
                pltpu.VMEM((S2, rows, T), F32),
                pltpu.VMEM((S, 2, T, width), BF16),
                pltpu.VMEM((rows, width), F32),
                pltpu.VMEM((rows, width), F32),
                pltpu.VMEM((rows, LANES), F32),
                pltpu.VMEM((rows, LANES), F32),
                pltpu.VMEM((8, LANES), F32),
                pltpu.VMEM((3, 8, LANES), F32),
                pltpu.VMEM((8, LANES), F32),
                pltpu.VMEM((3, 8, LANES), F32),
                pltpu.VMEM((8, LANES), F32),
                pltpu.VMEM((7, 8, LANES), F32),
                dma((S,)),
                dma((S2,)),
                dma((S2,)),
                dma,
                dma((len(groups),)),
                dma,
                dma,
                dma,
                dma,
                dma,
                dma,
                dma,
                dma,
            ],
            compiler_params=pltpu.CompilerParams(
                collective_id=0, has_side_effects=True, vmem_limit_bytes=52 * 2**20),
        )(hidden, lnf_gain.reshape(1, width), lnf_bias.reshape(1, width), next_tok.reshape(1, rows),
          eln_gain.reshape(1, width), eln_bias.reshape(1, width), emb_table)
        logp, log_sum, next_in = pl.pallas_call(
            finish_kernel,
            out_shape=(
                jax.ShapeDtypeStruct((rows, block), F32),
                jax.ShapeDtypeStruct((1, rows), F32),
                jax.ShapeDtypeStruct((rows, width), BF16),
            ),
            in_specs=[vmem, vmem, vmem],
            out_specs=(hbm, hbm, hbm),
            scratch_shapes=[
                pltpu.VMEM((rows, block), F32), pltpu.VMEM((1, rows), F32), dma, dma((2,))],
            compiler_params=pltpu.CompilerParams(vmem_limit_bytes=20 * 2**20),
        )(z, lse, nin)
        return logp, log_sum.reshape(rows), next_in

    return jax.shard_map(
        per_device,
        mesh=mesh,
        in_specs=(P("dp", "tp"), P("tp"), P("tp"), P("vp", "tp"), P("dp"), P("tp"), P("tp")),
        out_specs=(P("dp", ("vp", "tp")), P("dp"), P("dp", "tp")),
        check_vma=False,
    )
```

```python
import functools

import jax
import jax.numpy as jnp
from jax import lax
from jax.experimental import pallas as pl
from jax.experimental.pallas import tpu as pltpu
from jax.sharding import PartitionSpec as P

NORM_EPS = 1e-5
MESH = pl.DeviceIdType.MESH
F32 = jnp.float32
BF16 = jnp.bfloat16
LANES = 128


def diagonal(rows):
    return (lax.broadcasted_iota(jnp.int32, (rows, LANES), 0)
            == lax.broadcasted_iota(jnp.int32, (rows, LANES), 1))


def col_to_row(col):
    return jnp.sum(jnp.where(diagonal(col.shape[0]), col, jnp.zeros_like(col)), axis=0, keepdims=True)


def row_to_col(row, rows):
    return jnp.sum(jnp.where(diagonal(rows), row, jnp.zeros_like(row)), axis=1, keepdims=True)


def two_rows(first, second):
    sub = lax.broadcasted_iota(jnp.int32, (8, LANES), 0)
    return jnp.where(sub == 0, first, second)


def row_sums_tile(rows_f32):
    return two_rows(
        col_to_row(jnp.sum(rows_f32, axis=1, keepdims=True)),
        col_to_row(jnp.sum(rows_f32 * rows_f32, axis=1, keepdims=True)))


def norm_rows(rows_f32, totals, gain, bias, full_width):
    rows = rows_f32.shape[0]
    mean = totals[0:1, :] / full_width
    var = totals[1:2, :] / full_width - mean * mean
    rstd = lax.rsqrt(var + NORM_EPS)
    scaled = (rows_f32 - row_to_col(mean, rows)) * row_to_col(rstd, rows)
    return (scaled * gain + bias).astype(BF16)


def logits_kernel(
    cfg, hid_hbm, gain_hbm, bias_hbm, tok_hbm, egain_hbm, ebias_hbm, tab,
    z, lse, nin,
    hid, gain, bias, tok, egain, ebias, in_sem,
    hds_sem, hdr_sem, hxr_sem,
    xn, out, xrecv, drecv, stg, tbuf, pick, ypick, runmax, runsum,
    ln_send, ln_recv, eln_send, eln_recv, fin_send, fin_recv,
    tab_sem, dsend_sem, drecv_sem, xsend_sem, xrecv_sem, ysend_sem, yrecv_sem,
    lns_sem, lnr_sem, els_sem, elr_sem, fis_sem, fir_sem,
):
    n, T, B, S, S2, n0, full_width, head, groups = cfg
    rows = hid.shape[0]
    dp = lax.axis_index("dp")
    v = lax.axis_index("vp")
    t = lax.axis_index("tp")
    x = lax.div(t, 2)
    c = lax.rem(t, 2)

    def peer(d):
        pv = 1 - v if d >= 4 else v
        px = 1 - x if (d // 2) % 2 else x
        pc = 1 - c if d % 2 else c
        return (dp, pv, 2 * px + pc)

    def start_table(j):
        a = lax.div(j, n)
        i = j - a * n
        xx = (1 - x) + a * (2 * x - 1)
        for w in range(2):
            cc = 1 - c if w == 0 else c
            row = pl.multiple_of((2 * xx + cc) * B + i * T, LANES)
            slot = lax.rem(j, S)
            pltpu.make_async_copy(tab.at[pl.ds(row, T)], tbuf.at[slot, w], tab_sem.at[slot]).start()

    def wait_table(j):
        slot = lax.rem(j, S)
        pltpu.make_async_copy(tbuf.at[slot], tbuf.at[slot], tab_sem.at[slot]).wait()

    def first_row(j, w):
        a = lax.div(j, n)
        i = j - a * n
        xx = (1 - x) + a * (2 * x - 1)
        cc = 1 - c if w == 0 else c
        return v * (4 * B) + (2 * xx + cc) * B + i * T

    def d2d_copy(j):
        slot = lax.rem(j, S2)
        return pltpu.make_async_remote_copy(
            src_ref=stg.at[slot], dst_ref=drecv.at[slot],
            send_sem=dsend_sem.at[slot], recv_sem=drecv_sem.at[slot],
            device_id=peer(1), device_id_type=MESH)

    def x_copy(g):
        first, last = groups[g]
        part = pl.ds(first, last - first)
        return pltpu.make_async_remote_copy(
            src_ref=out.at[part], dst_ref=xrecv.at[part],
            send_sem=xsend_sem, recv_sem=xrecv_sem.at[g],
            device_id=peer(2), device_id_type=MESH)

    def small_copy(src, dst, ssem, rsem, d):
        return pltpu.make_async_remote_copy(
            src_ref=src, dst_ref=dst.at[d - 1], send_sem=ssem, recv_sem=rsem,
            device_id=peer(d), device_id_type=MESH)

    def wait_small(dst, ssem, rsem):
        both = pltpu.make_async_remote_copy(
            src_ref=dst, dst_ref=dst, send_sem=ssem, recv_sem=rsem,
            device_id=peer(1), device_id_type=MESH)
        both.wait_recv()
        both.wait_send()

    barrier = pltpu.get_barrier_semaphore()
    for d in (4, 2, 3, 1):
        pl.semaphore_signal(barrier, inc=1, device_id=peer(d), device_id_type=MESH)

    pairs = ((hid_hbm, hid), (gain_hbm, gain), (bias_hbm, bias), (tok_hbm, tok),
             (egain_hbm, egain), (ebias_hbm, ebias))
    loads = [pltpu.make_async_copy(src, dst, in_sem.at[k]) for k, (src, dst) in enumerate(pairs)]
    for load in loads:
        load.start()
    for j in range(S):
        start_table(j)

    loads[0].wait()
    hid_f32 = hid[...].astype(F32)
    ln_send[...] = row_sums_tile(hid_f32)
    pl.semaphore_wait(barrier, 4)

    for d in (2, 3, 1):
        small_copy(ln_send, ln_recv, lns_sem, lnr_sem, d).start()
    for load in loads[1:]:
        load.wait()
    eye = (lax.broadcasted_iota(jnp.int32, (rows, rows), 0)
           == lax.broadcasted_iota(jnp.int32, (rows, rows), 1))
    tok_col = jnp.sum(
        jnp.where(eye, tok[...].astype(F32), 0.0), axis=1, keepdims=True).astype(jnp.int32)
    pick[...] = jnp.zeros_like(pick)
    runmax[...] = jnp.full(runmax.shape, -jnp.inf, F32)
    runsum[...] = jnp.zeros_like(runsum)
    wait_table(0)
    totals = ln_send[...]
    wait_small(ln_recv, lns_sem, lnr_sem)
    for d in range(3):
        totals = totals + ln_recv[d]
    xn[...] = norm_rows(hid_f32, totals, gain[...], bias[...], full_width)

    def matmul(j, w):
        slot = lax.rem(j, S)
        return lax.dot_general(
            xn[...], tbuf[slot, w], (((1,), (1,)), ((), ())), preferred_element_type=F32)

    def pick_rows(j):
        slot = lax.rem(j, S)
        total = pick[...]
        for w in range(2):
            local = tok_col - first_row(j, w)
            hot = (lax.broadcasted_iota(jnp.int32, (rows, T), 1) == local).astype(F32).astype(BF16)
            total = total + jnp.dot(hot, tbuf[slot, w], preferred_element_type=F32)
        pick[...] = total

    def zcols(i):
        return pl.ds(pl.multiple_of(i * T, LANES), T)

    def send_half(j):
        wait_table(j)

        @pl.when(j > S2)
        def _():
            d2d_copy(j - S2).wait_send()

        stg[lax.rem(j, S2)] = matmul(j, 0)

    def combine_out(i):
        d2d_copy(i).wait_recv()
        out[i] = out[i] + drecv[lax.rem(i, S2)]

    def refill(j):
        @pl.when(j + S < 2 * n)
        def _():
            start_table(j + S)

    def head_d2d(k):
        cols = pl.ds(head[k], head[k + 1] - head[k])
        return pltpu.make_async_remote_copy(
            src_ref=stg.at[0, :, cols], dst_ref=drecv.at[0, :, cols],
            send_sem=hds_sem, recv_sem=hdr_sem.at[k],
            device_id=peer(1), device_id_type=MESH)

    def head_x(k):
        cols = pl.ds(head[k], head[k + 1] - head[k])
        return pltpu.make_async_remote_copy(
            src_ref=out.at[0, :, cols], dst_ref=xrecv.at[0, :, cols],
            send_sem=xsend_sem, recv_sem=hxr_sem,
            device_id=peer(2), device_id_type=MESH)

    def head_matmul(k, w):
        return lax.dot_general(
            xn[...], tbuf[0, w, head[k]:head[k + 1], :], (((1,), (1,)), ((), ())),
            preferred_element_type=F32)

    def head_combine(k):
        head_d2d(k).wait_recv()
        cols = slice(head[k], head[k + 1])
        out[0, :, cols] = out[0, :, cols] + drecv[0, :, cols]

    pieces = len(head) - 1

    def head_give(k):
        stg[0, :, head[k]:head[k + 1]] = head_matmul(k, 0)

    def head_keep(k):
        out[0, :, head[k]:head[k + 1]] = head_matmul(k, 1)

    @pl.when(c == 0)
    def _():
        for k in range(pieces):
            head_keep(k)
        head_give(0)
        for k in range(pieces):
            head_combine(k)
            if k + 1 < pieces:
                head_give(k + 1)
            head_d2d(k).start()
            head_x(k).start()
        pick_rows(0)

    @pl.when(c == 1)
    def _():
        for k in range(pieces):
            head_give(k)
            if k >= 1:
                head_d2d(k - 1).start()
        head_keep(0)
        head_d2d(pieces - 1).start()
        for k in range(1, pieces):
            head_keep(k)
        pick_rows(0)
        for k in range(pieces):
            head_combine(k)

    refill(0)
    pltpu.make_async_remote_copy(
        src_ref=stg.at[0], dst_ref=drecv.at[0], send_sem=hds_sem, recv_sem=hdr_sem.at[0],
        device_id=peer(1), device_id_type=MESH).wait_send()

    @pl.loop(1, n)
    def _(j):
        @pl.when(jnp.logical_and(c == 1, j == 2))
        def _():
            for k in range(pieces):
                head_x(k).start()

        @pl.when(j >= 2)
        def _():
            combine_out(j - 1)

        send_half(j)

        for g in range(n0):
            @pl.when(j == groups[g][1])
            def _():
                x_copy(g).start()

        d2d_copy(j).start()

        out[j] = matmul(j, 1)
        pick_rows(j)
        refill(j)

    @pl.loop(n, 2 * n)
    def _(j):
        send_half(j)

        @pl.when(j == n)
        def _():
            combine_out(n - 1)

        @pl.when(j > n)
        def _():
            d2d_copy(j - 1).wait_recv()
            z[:, zcols(j - 1 - n)] = z[:, zcols(j - 1 - n)] + drecv[lax.rem(j - 1, S2)]

        d2d_copy(j).start()
        z[:, zcols(j - n)] = matmul(j, 1)
        pick_rows(j)
        refill(j)

    d2d_copy(2 * n - 1).wait_recv()
    z[:, zcols(n - 1)] = z[:, zcols(n - 1)] + drecv[(2 * n - 1) % S2]

    ycopy = pltpu.make_async_remote_copy(
        src_ref=pick, dst_ref=ypick, send_sem=ysend_sem, recv_sem=yrecv_sem,
        device_id=peer(4), device_id_type=MESH)
    ycopy.start()
    ycopy.wait()
    tok_rows = pick[...] + ypick[...]
    eln_send[...] = row_sums_tile(tok_rows)
    for d in range(1, 4):
        small_copy(eln_send, eln_recv, els_sem, elr_sem, d).start()
    for g in range(n0, len(groups)):
        x_copy(g).start()

    def absorb(i):
        m_old = runmax[...]
        m_new = m_old
        for k in range(T // LANES):
            cols = pl.ds(pl.multiple_of(i * T, LANES) + k * LANES, LANES)
            val = z[:, cols] + xrecv[i, :, k * LANES:(k + 1) * LANES]
            z[:, cols] = val
            m_new = jnp.maximum(m_new, val)
        s_new = runsum[...] * jnp.exp(m_old - m_new)
        for k in range(T // LANES):
            cols = pl.ds(pl.multiple_of(i * T, LANES) + k * LANES, LANES)
            s_new = s_new + jnp.exp(z[:, cols] - m_new)
        runmax[...] = m_new
        runsum[...] = s_new

    pltpu.make_async_remote_copy(
        src_ref=out.at[0], dst_ref=xrecv.at[0], send_sem=xsend_sem, recv_sem=hxr_sem,
        device_id=peer(2), device_id_type=MESH).wait_recv()

    absorb(0)
    for g, (first, last) in enumerate(groups):
        x_copy(g).wait_recv()

        @pl.loop(first, last)
        def _(i):
            absorb(i)

    top = jnp.max(runmax[...], axis=1, keepdims=True)
    exp_sum = jnp.sum(runsum[...] * jnp.exp(runmax[...] - top), axis=1, keepdims=True)
    fin_send[...] = two_rows(col_to_row(top), col_to_row(exp_sum))
    for d in (6, 7, 5, 4, 2, 3, 1):
        small_copy(fin_send, fin_recv, fis_sem, fir_sem, d).start()

    totals = eln_send[...]
    wait_small(eln_recv, els_sem, elr_sem)
    for d in range(3):
        totals = totals + eln_recv[d]
    nin[...] = norm_rows(pick[...] + ypick[...], totals, egain[...], ebias[...], full_width)

    pltpu.make_async_remote_copy(
        src_ref=out, dst_ref=xrecv, send_sem=xsend_sem, recv_sem=hxr_sem,
        device_id=peer(2), device_id_type=MESH).wait_send()

    @pl.loop(2 * n - S2, 2 * n)
    def _(j):
        d2d_copy(j).wait_send()

    tiles = [fin_send[...]]
    wait_small(fin_recv, fis_sem, fir_sem)
    for d in range(7):
        tiles.append(fin_recv[d])
    best = tiles[0][0:1, :]
    for tile in tiles[1:]:
        best = jnp.maximum(best, tile[0:1, :])
    total = jnp.zeros_like(best)
    for tile in tiles:
        total = total + tile[1:2, :] * jnp.exp(tile[0:1, :] - best)
    lse[...] = jnp.broadcast_to(best + jnp.log(total), lse.shape)


def finish_kernel(z, lse, nin, logp, log_sum, next_in, buf, row, sem, small_sem):
    rows, width = z.shape
    col = row_to_col(lse[0:1, :], rows)
    cuts = [0, 16 * LANES, 48 * LANES, 112 * LANES, width]
    parts = [(0, lo, hi) for lo, hi in zip(cuts, cuts[1:])]
    parts += [(r, 0, width) for r in range(8, rows, 8)]

    def put(b):
        r, lo, hi = parts[b]
        part = (pl.ds(r, 8), pl.ds(lo, hi - lo))
        return pltpu.make_async_copy(buf.at[part], logp.at[part], sem)

    row[...] = lse[0:1, 0:rows]
    nin_copy = pltpu.make_async_copy(nin, next_in, small_sem.at[0])
    row_copy = pltpu.make_async_copy(row, log_sum, small_sem.at[1])
    for b, (r, lo, hi) in enumerate(parts):
        buf[r:r + 8, lo:hi] = z[r:r + 8, lo:hi] - col[r:r + 8, :]
        if b >= 1:
            put(b - 1).start()
        if b == 3:
            nin_copy.start()
            row_copy.start()
    put(len(parts) - 1).start()
    nin_copy.wait()
    row_copy.wait()
    pltpu.make_async_copy(buf, logp, sem).wait()


def solution(mesh):
    tp_size = mesh.shape["tp"]

    def per_device(hidden, lnf_gain, lnf_bias, emb_table, next_tok, eln_gain, eln_bias):
        rows, width = hidden.shape
        block = emb_table.shape[0] // tp_size
        T = 7 * LANES
        n = block // T
        S, S2, n0 = 3, 3, 5
        sizes = (1, 2, 5, 10, 10, 5, 1)
        groups, at = [], 1
        for size in sizes:
            groups.append((at, at + size))
            at += size
        head = (0, LANES, 3 * LANES, T)
        cfg = (n, T, block, S, S2, n0, float(width * tp_size), head, tuple(groups))
        vmem = pl.BlockSpec(memory_space=pltpu.VMEM)
        hbm = pl.BlockSpec(memory_space=pl.ANY)
        dma = pltpu.SemaphoreType.DMA
        z, lse, nin = pl.pallas_call(
            functools.partial(logits_kernel, cfg),
            out_shape=(
                pltpu.VMEM((rows, block), F32),
                pltpu.VMEM((8, LANES), F32),
                pltpu.VMEM((rows, width), BF16),
            ),
            in_specs=[hbm] * 7,
            out_specs=(vmem, vmem, vmem),
            scratch_shapes=[
                pltpu.VMEM((rows, width), BF16),
                pltpu.VMEM((1, width), F32),
                pltpu.VMEM((1, width), F32),
                pltpu.VMEM((1, rows), jnp.int32),
                pltpu.VMEM((1, width), F32),
                pltpu.VMEM((1, width), F32),
                dma((6,)),
                dma,
                dma((len(head) - 1,)),
                dma,
                pltpu.VMEM((rows, width), BF16),
                pltpu.VMEM((n, rows, T), F32),
                pltpu.VMEM((n, rows, T), F32),
                pltpu.VMEM((S2, rows, T), F32),
                pltpu.VMEM((S2, rows, T), F32),
                pltpu.VMEM((S, 2, T, width), BF16),
                pltpu.VMEM((rows, width), F32),
                pltpu.VMEM((rows, width), F32),
                pltpu.VMEM((rows, LANES), F32),
                pltpu.VMEM((rows, LANES), F32),
                pltpu.VMEM((8, LANES), F32),
                pltpu.VMEM((3, 8, LANES), F32),
                pltpu.VMEM((8, LANES), F32),
                pltpu.VMEM((3, 8, LANES), F32),
                pltpu.VMEM((8, LANES), F32),
                pltpu.VMEM((7, 8, LANES), F32),
                dma((S,)),
                dma((S2,)),
                dma((S2,)),
                dma,
                dma((len(groups),)),
                dma,
                dma,
                dma,
                dma,
                dma,
                dma,
                dma,
                dma,
            ],
            compiler_params=pltpu.CompilerParams(
                collective_id=0, has_side_effects=True, vmem_limit_bytes=52 * 2**20),
        )(hidden, lnf_gain.reshape(1, width), lnf_bias.reshape(1, width), next_tok.reshape(1, rows),
          eln_gain.reshape(1, width), eln_bias.reshape(1, width), emb_table)
        logp, log_sum, next_in = pl.pallas_call(
            finish_kernel,
            out_shape=(
                jax.ShapeDtypeStruct((rows, block), F32),
                jax.ShapeDtypeStruct((1, rows), F32),
                jax.ShapeDtypeStruct((rows, width), BF16),
            ),
            in_specs=[vmem, vmem, vmem],
            out_specs=(hbm, hbm, hbm),
            scratch_shapes=[
                pltpu.VMEM((rows, block), F32), pltpu.VMEM((1, rows), F32), dma, dma((2,))],
            compiler_params=pltpu.CompilerParams(vmem_limit_bytes=20 * 2**20),
        )(z, lse, nin)
        return logp, log_sum.reshape(rows), next_in

    return jax.shard_map(
        per_device,
        mesh=mesh,
        in_specs=(P("dp", "tp"), P("tp"), P("tp"), P("vp", "tp"), P("dp"), P("tp"), P("tp")),
        out_specs=(P("dp", ("vp", "tp")), P("dp"), P("dp", "tp")),
        check_vma=False,
    )
```

```python
import functools

import jax
import jax.numpy as jnp
from jax import lax
from jax.experimental import pallas as pl
from jax.experimental.pallas import tpu as pltpu
from jax.sharding import PartitionSpec as P

NORM_EPS = 1e-5
MESH = pl.DeviceIdType.MESH
F32 = jnp.float32
BF16 = jnp.bfloat16
LANES = 128


def diagonal(rows):
    return (lax.broadcasted_iota(jnp.int32, (rows, LANES), 0)
            == lax.broadcasted_iota(jnp.int32, (rows, LANES), 1))


def col_to_row(col):
    return jnp.sum(jnp.where(diagonal(col.shape[0]), col, jnp.zeros_like(col)), axis=0, keepdims=True)


def row_to_col(row, rows):
    return jnp.sum(jnp.where(diagonal(rows), row, jnp.zeros_like(row)), axis=1, keepdims=True)


def two_rows(first, second):
    sub = lax.broadcasted_iota(jnp.int32, (8, LANES), 0)
    return jnp.where(sub == 0, first, second)


def row_sums_tile(rows_f32):
    return two_rows(
        col_to_row(jnp.sum(rows_f32, axis=1, keepdims=True)),
        col_to_row(jnp.sum(rows_f32 * rows_f32, axis=1, keepdims=True)))


def norm_rows(rows_f32, totals, gain, bias, full_width):
    rows = rows_f32.shape[0]
    mean = totals[0:1, :] / full_width
    var = totals[1:2, :] / full_width - mean * mean
    rstd = lax.rsqrt(var + NORM_EPS)
    scaled = (rows_f32 - row_to_col(mean, rows)) * row_to_col(rstd, rows)
    return (scaled * gain + bias).astype(BF16)


def logits_kernel(
    cfg, hid_hbm, gain_hbm, bias_hbm, tok_hbm, egain_hbm, ebias_hbm, tab,
    z, lse, nin,
    hid, gain, bias, tok, egain, ebias, in_sem,
    hds_sem, hdr_sem, hxr_sem, extra, extra_sem,
    xn, out, xrecv, drecv, stg, tbuf, pick, ypick, runmax, runsum,
    ln_send, ln_recv, eln_send, eln_recv, fin_send, fin_recv,
    tab_sem, dsend_sem, drecv_sem, xsend_sem, xrecv_sem, ysend_sem, yrecv_sem,
    lns_sem, lnr_sem, els_sem, elr_sem, fis_sem, fir_sem,
):
    n, T, B, S, S2, n0, full_width, head, groups = cfg
    rows = hid.shape[0]
    dp = lax.axis_index("dp")
    v = lax.axis_index("vp")
    t = lax.axis_index("tp")
    x = lax.div(t, 2)
    c = lax.rem(t, 2)

    def peer(d):
        pv = 1 - v if d >= 4 else v
        px = 1 - x if (d // 2) % 2 else x
        pc = 1 - c if d % 2 else c
        return (dp, pv, 2 * px + pc)

    def start_table(j):
        a = lax.div(j, n)
        i = j - a * n
        xx = (1 - x) + a * (2 * x - 1)
        for w in range(2):
            cc = 1 - c if w == 0 else c
            row = pl.multiple_of((2 * xx + cc) * B + i * T, LANES)
            slot = lax.rem(j, S)
            pltpu.make_async_copy(tab.at[pl.ds(row, T)], tbuf.at[slot, w], tab_sem.at[slot]).start()

    def wait_table(j):
        slot = lax.rem(j, S)
        pltpu.make_async_copy(tbuf.at[slot], tbuf.at[slot], tab_sem.at[slot]).wait()

    def first_row(j, w):
        a = lax.div(j, n)
        i = j - a * n
        xx = (1 - x) + a * (2 * x - 1)
        cc = 1 - c if w == 0 else c
        return v * (4 * B) + (2 * xx + cc) * B + i * T

    def d2d_copy(j):
        slot = lax.rem(j, S2)
        return pltpu.make_async_remote_copy(
            src_ref=stg.at[slot], dst_ref=drecv.at[slot],
            send_sem=dsend_sem.at[slot], recv_sem=drecv_sem.at[slot],
            device_id=peer(1), device_id_type=MESH)

    def x_copy(g):
        first, last = groups[g]
        part = pl.ds(first, last - first)
        return pltpu.make_async_remote_copy(
            src_ref=out.at[part], dst_ref=xrecv.at[part],
            send_sem=xsend_sem, recv_sem=xrecv_sem.at[g],
            device_id=peer(2), device_id_type=MESH)

    def small_copy(src, dst, ssem, rsem, d):
        return pltpu.make_async_remote_copy(
            src_ref=src, dst_ref=dst.at[d - 1], send_sem=ssem, recv_sem=rsem,
            device_id=peer(d), device_id_type=MESH)

    def wait_small(dst, ssem, rsem):
        both = pltpu.make_async_remote_copy(
            src_ref=dst, dst_ref=dst, send_sem=ssem, recv_sem=rsem,
            device_id=peer(1), device_id_type=MESH)
        both.wait_recv()
        both.wait_send()

    barrier = pltpu.get_barrier_semaphore()
    for d in (4, 2, 3, 1):
        pl.semaphore_signal(barrier, inc=1, device_id=peer(d), device_id_type=MESH)

    pairs = ((hid_hbm, hid), (gain_hbm, gain), (bias_hbm, bias), (tok_hbm, tok),
             (egain_hbm, egain), (ebias_hbm, ebias))
    loads = [pltpu.make_async_copy(src, dst, in_sem.at[k]) for k, (src, dst) in enumerate(pairs)]
    for load in loads:
        load.start()
    for j in range(S):
        start_table(j)

    loads[0].wait()
    hid_f32 = hid[...].astype(F32)
    ln_send[...] = row_sums_tile(hid_f32)
    pl.semaphore_wait(barrier, 4)

    for d in (2, 3, 1):
        small_copy(ln_send, ln_recv, lns_sem, lnr_sem, d).start()
    for load in loads[1:]:
        load.wait()
    eye = (lax.broadcasted_iota(jnp.int32, (rows, rows), 0)
           == lax.broadcasted_iota(jnp.int32, (rows, rows), 1))
    tok_col = jnp.sum(
        jnp.where(eye, tok[...].astype(F32), 0.0), axis=1, keepdims=True).astype(jnp.int32)
    pick[...] = jnp.zeros_like(pick)
    runmax[...] = jnp.full(runmax.shape, -jnp.inf, F32)
    runsum[...] = jnp.zeros_like(runsum)
    wait_table(0)
    totals = ln_send[...]
    wait_small(ln_recv, lns_sem, lnr_sem)
    for d in range(3):
        totals = totals + ln_recv[d]
    xn[...] = norm_rows(hid_f32, totals, gain[...], bias[...], full_width)

    def matmul(j, w):
        slot = lax.rem(j, S)
        return lax.dot_general(
            xn[...], tbuf[slot, w], (((1,), (1,)), ((), ())), preferred_element_type=F32)

    def pick_rows(j):
        slot = lax.rem(j, S)
        total = pick[...]
        for w in range(2):
            local = tok_col - first_row(j, w)
            hot = (lax.broadcasted_iota(jnp.int32, (rows, T), 1) == local).astype(F32).astype(BF16)
            total = total + jnp.dot(hot, tbuf[slot, w], preferred_element_type=F32)
        pick[...] = total

    def zcols(i):
        return pl.ds(pl.multiple_of(i * T, LANES), T)

    def send_half(j):
        wait_table(j)

        @pl.when(j > S2)
        def _():
            d2d_copy(j - S2).wait_send()

        stg[lax.rem(j, S2)] = matmul(j, 0)

    def combine_out(i):
        d2d_copy(i).wait_recv()
        out[i] = out[i] + drecv[lax.rem(i, S2)]

    def refill(j):
        @pl.when(j + S < 2 * n)
        def _():
            start_table(j + S)

    def head_d2d(k):
        cols = pl.ds(head[k], head[k + 1] - head[k])
        return pltpu.make_async_remote_copy(
            src_ref=stg.at[0, :, cols], dst_ref=drecv.at[0, :, cols],
            send_sem=hds_sem, recv_sem=hdr_sem.at[k],
            device_id=peer(1), device_id_type=MESH)

    def head_x(k):
        cols = pl.ds(head[k], head[k + 1] - head[k])
        return pltpu.make_async_remote_copy(
            src_ref=out.at[0, :, cols], dst_ref=xrecv.at[0, :, cols],
            send_sem=xsend_sem, recv_sem=hxr_sem,
            device_id=peer(2), device_id_type=MESH)

    def head_matmul(k, w):
        return lax.dot_general(
            xn[...], tbuf[0, w, head[k]:head[k + 1], :], (((1,), (1,)), ((), ())),
            preferred_element_type=F32)

    def head_combine(k):
        head_d2d(k).wait_recv()
        cols = slice(head[k], head[k + 1])
        out[0, :, cols] = out[0, :, cols] + drecv[0, :, cols]

    pieces = len(head) - 1

    def head_give(k):
        stg[0, :, head[k]:head[k + 1]] = head_matmul(k, 0)

    def head_keep(k):
        out[0, :, head[k]:head[k + 1]] = head_matmul(k, 1)

    part_copy = pltpu.make_async_remote_copy(
        src_ref=stg.at[0, :, pl.ds(head[0], head[1])], dst_ref=extra,
        send_sem=hds_sem, recv_sem=extra_sem, device_id=peer(3), device_id_type=MESH)

    @pl.when(c == 0)
    def _():
        head_keep(0)
        head_keep(1)
        head_x(0).start()
        for k in range(2, pieces):
            head_keep(k)
        head_give(0)
        for k in range(1, pieces):
            head_combine(k)
            head_give(k)
            head_d2d(k - 1).start()
            head_x(k).start()
        head_d2d(pieces - 1).start()
        pick_rows(0)

    @pl.when(c == 1)
    def _():
        head_give(0)
        head_give(1)
        part_copy.start()
        for k in range(2, pieces):
            head_give(k)
            head_d2d(k - 1).start()
        head_keep(0)
        head_d2d(pieces - 1).start()
        for k in range(1, pieces):
            head_keep(k)
        pick_rows(0)
        for k in range(pieces):
            head_combine(k)

    refill(0)
    pltpu.make_async_remote_copy(
        src_ref=stg.at[0], dst_ref=drecv.at[0], send_sem=hds_sem, recv_sem=hdr_sem.at[0],
        device_id=peer(1), device_id_type=MESH).wait_send()

    @pl.loop(1, n)
    def _(j):
        @pl.when(j >= 2)
        def _():
            combine_out(j - 1)

        send_half(j)

        for g in range(n0):
            @pl.when(j == groups[g][1])
            def _():
                x_copy(g).start()

        d2d_copy(j).start()

        @pl.when(jnp.logical_and(c == 1, j == 1))
        def _():
            for k in range(pieces):
                head_x(k).start()

        out[j] = matmul(j, 1)
        pick_rows(j)
        refill(j)

    @pl.loop(n, 2 * n)
    def _(j):
        send_half(j)

        @pl.when(j == n)
        def _():
            combine_out(n - 1)

        @pl.when(j > n)
        def _():
            d2d_copy(j - 1).wait_recv()
            z[:, zcols(j - 1 - n)] = z[:, zcols(j - 1 - n)] + drecv[lax.rem(j - 1, S2)]

        d2d_copy(j).start()
        z[:, zcols(j - n)] = matmul(j, 1)
        pick_rows(j)
        refill(j)

    d2d_copy(2 * n - 1).wait_recv()
    z[:, zcols(n - 1)] = z[:, zcols(n - 1)] + drecv[(2 * n - 1) % S2]

    ycopy = pltpu.make_async_remote_copy(
        src_ref=pick, dst_ref=ypick, send_sem=ysend_sem, recv_sem=yrecv_sem,
        device_id=peer(4), device_id_type=MESH)
    ycopy.start()
    ycopy.wait()
    tok_rows = pick[...] + ypick[...]
    eln_send[...] = row_sums_tile(tok_rows)
    for d in range(1, 4):
        small_copy(eln_send, eln_recv, els_sem, elr_sem, d).start()
    for g in range(n0, len(groups)):
        x_copy(g).start()

    def absorb(i):
        m_old = runmax[...]
        m_new = m_old
        for k in range(T // LANES):
            cols = pl.ds(pl.multiple_of(i * T, LANES) + k * LANES, LANES)
            val = z[:, cols] + xrecv[i, :, k * LANES:(k + 1) * LANES]
            z[:, cols] = val
            m_new = jnp.maximum(m_new, val)
        s_new = runsum[...] * jnp.exp(m_old - m_new)
        for k in range(T // LANES):
            cols = pl.ds(pl.multiple_of(i * T, LANES) + k * LANES, LANES)
            s_new = s_new + jnp.exp(z[:, cols] - m_new)
        runmax[...] = m_new
        runsum[...] = s_new

    pltpu.make_async_remote_copy(
        src_ref=out.at[0], dst_ref=xrecv.at[0], send_sem=xsend_sem, recv_sem=hxr_sem,
        device_id=peer(2), device_id_type=MESH).wait_recv()

    @pl.when(c == 0)
    def _():
        part_copy.wait_recv()
        xrecv[0, :, head[0]:head[1]] = xrecv[0, :, head[0]:head[1]] + extra[...]

    absorb(0)
    for g, (first, last) in enumerate(groups):
        x_copy(g).wait_recv()

        @pl.loop(first, last)
        def _(i):
            absorb(i)

    top = jnp.max(runmax[...], axis=1, keepdims=True)
    exp_sum = jnp.sum(runsum[...] * jnp.exp(runmax[...] - top), axis=1, keepdims=True)
    fin_send[...] = two_rows(col_to_row(top), col_to_row(exp_sum))
    for d in (6, 7, 5, 4, 2, 3, 1):
        small_copy(fin_send, fin_recv, fis_sem, fir_sem, d).start()

    totals = eln_send[...]
    wait_small(eln_recv, els_sem, elr_sem)
    for d in range(3):
        totals = totals + eln_recv[d]
    nin[...] = norm_rows(pick[...] + ypick[...], totals, egain[...], ebias[...], full_width)

    pltpu.make_async_remote_copy(
        src_ref=out, dst_ref=xrecv, send_sem=xsend_sem, recv_sem=hxr_sem,
        device_id=peer(2), device_id_type=MESH).wait_send()

    @pl.loop(2 * n - S2, 2 * n)
    def _(j):
        d2d_copy(j).wait_send()

    tiles = [fin_send[...]]
    wait_small(fin_recv, fis_sem, fir_sem)
    for d in range(7):
        tiles.append(fin_recv[d])
    best = tiles[0][0:1, :]
    for tile in tiles[1:]:
        best = jnp.maximum(best, tile[0:1, :])
    total = jnp.zeros_like(best)
    for tile in tiles:
        total = total + tile[1:2, :] * jnp.exp(tile[0:1, :] - best)
    lse[...] = jnp.broadcast_to(best + jnp.log(total), lse.shape)


def finish_kernel(z, lse, nin, logp, log_sum, next_in, buf, row, sem, small_sem):
    rows, width = z.shape
    col = row_to_col(lse[0:1, :], rows)
    cuts = [0, 16 * LANES, 48 * LANES, 112 * LANES, width]
    parts = [(0, lo, hi) for lo, hi in zip(cuts, cuts[1:])]
    parts += [(r, 0, width) for r in range(8, rows, 8)]

    def put(b):
        r, lo, hi = parts[b]
        part = (pl.ds(r, 8), pl.ds(lo, hi - lo))
        return pltpu.make_async_copy(buf.at[part], logp.at[part], sem)

    row[...] = lse[0:1, 0:rows]
    nin_copy = pltpu.make_async_copy(nin, next_in, small_sem.at[0])
    row_copy = pltpu.make_async_copy(row, log_sum, small_sem.at[1])
    for b, (r, lo, hi) in enumerate(parts):
        buf[r:r + 8, lo:hi] = z[r:r + 8, lo:hi] - col[r:r + 8, :]
        if b >= 1:
            put(b - 1).start()
        if b == 3:
            nin_copy.start()
            row_copy.start()
    put(len(parts) - 1).start()
    nin_copy.wait()
    row_copy.wait()
    pltpu.make_async_copy(buf, logp, sem).wait()


def solution(mesh):
    tp_size = mesh.shape["tp"]

    def per_device(hidden, lnf_gain, lnf_bias, emb_table, next_tok, eln_gain, eln_bias):
        rows, width = hidden.shape
        block = emb_table.shape[0] // tp_size
        T = 7 * LANES
        n = block // T
        S, S2, n0 = 3, 3, 5
        sizes = (1, 2, 5, 10, 10, 5, 1)
        groups, at = [], 1
        for size in sizes:
            groups.append((at, at + size))
            at += size
        head = (0, 2 * LANES, 4 * LANES, T)
        cfg = (n, T, block, S, S2, n0, float(width * tp_size), head, tuple(groups))
        vmem = pl.BlockSpec(memory_space=pltpu.VMEM)
        hbm = pl.BlockSpec(memory_space=pl.ANY)
        dma = pltpu.SemaphoreType.DMA
        z, lse, nin = pl.pallas_call(
            functools.partial(logits_kernel, cfg),
            out_shape=(
                pltpu.VMEM((rows, block), F32),
                pltpu.VMEM((8, LANES), F32),
                pltpu.VMEM((rows, width), BF16),
            ),
            in_specs=[hbm] * 7,
            out_specs=(vmem, vmem, vmem),
            scratch_shapes=[
                pltpu.VMEM((rows, width), BF16),
                pltpu.VMEM((1, width), F32),
                pltpu.VMEM((1, width), F32),
                pltpu.VMEM((1, rows), jnp.int32),
                pltpu.VMEM((1, width), F32),
                pltpu.VMEM((1, width), F32),
                dma((6,)),
                dma,
                dma((len(head) - 1,)),
                dma,
                pltpu.VMEM((rows, head[1]), F32),
                dma,
                pltpu.VMEM((rows, width), BF16),
                pltpu.VMEM((n, rows, T), F32),
                pltpu.VMEM((n, rows, T), F32),
                pltpu.VMEM((S2, rows, T), F32),
                pltpu.VMEM((S2, rows, T), F32),
                pltpu.VMEM((S, 2, T, width), BF16),
                pltpu.VMEM((rows, width), F32),
                pltpu.VMEM((rows, width), F32),
                pltpu.VMEM((rows, LANES), F32),
                pltpu.VMEM((rows, LANES), F32),
                pltpu.VMEM((8, LANES), F32),
                pltpu.VMEM((3, 8, LANES), F32),
                pltpu.VMEM((8, LANES), F32),
                pltpu.VMEM((3, 8, LANES), F32),
                pltpu.VMEM((8, LANES), F32),
                pltpu.VMEM((7, 8, LANES), F32),
                dma((S,)),
                dma((S2,)),
                dma((S2,)),
                dma,
                dma((len(groups),)),
                dma,
                dma,
                dma,
                dma,
                dma,
                dma,
                dma,
                dma,
            ],
            compiler_params=pltpu.CompilerParams(
                collective_id=0, has_side_effects=True, vmem_limit_bytes=52 * 2**20),
        )(hidden, lnf_gain.reshape(1, width), lnf_bias.reshape(1, width), next_tok.reshape(1, rows),
          eln_gain.reshape(1, width), eln_bias.reshape(1, width), emb_table)
        logp, log_sum, next_in = pl.pallas_call(
            finish_kernel,
            out_shape=(
                jax.ShapeDtypeStruct((rows, block), F32),
                jax.ShapeDtypeStruct((1, rows), F32),
                jax.ShapeDtypeStruct((rows, width), BF16),
            ),
            in_specs=[vmem, vmem, vmem],
            out_specs=(hbm, hbm, hbm),
            scratch_shapes=[
                pltpu.VMEM((rows, block), F32), pltpu.VMEM((1, rows), F32), dma, dma((2,))],
            compiler_params=pltpu.CompilerParams(vmem_limit_bytes=20 * 2**20),
        )(z, lse, nin)
        return logp, log_sum.reshape(rows), next_in

    return jax.shard_map(
        per_device,
        mesh=mesh,
        in_specs=(P("dp", "tp"), P("tp"), P("tp"), P("vp", "tp"), P("dp"), P("tp"), P("tp")),
        out_specs=(P("dp", ("vp", "tp")), P("dp"), P("dp", "tp")),
        check_vma=False,
    )
```

```python
import functools

import jax
import jax.numpy as jnp
from jax import lax
from jax.experimental import pallas as pl
from jax.experimental.pallas import tpu as pltpu
from jax.sharding import PartitionSpec as P

NORM_EPS = 1e-5
MESH = pl.DeviceIdType.MESH
F32 = jnp.float32
BF16 = jnp.bfloat16
LANES = 128


def diagonal(rows):
    return (lax.broadcasted_iota(jnp.int32, (rows, LANES), 0)
            == lax.broadcasted_iota(jnp.int32, (rows, LANES), 1))


def col_to_row(col):
    return jnp.sum(jnp.where(diagonal(col.shape[0]), col, jnp.zeros_like(col)), axis=0, keepdims=True)


def row_to_col(row, rows):
    return jnp.sum(jnp.where(diagonal(rows), row, jnp.zeros_like(row)), axis=1, keepdims=True)


def two_rows(first, second):
    sub = lax.broadcasted_iota(jnp.int32, (8, LANES), 0)
    return jnp.where(sub == 0, first, second)


def row_sums_tile(rows_f32):
    return two_rows(
        col_to_row(jnp.sum(rows_f32, axis=1, keepdims=True)),
        col_to_row(jnp.sum(rows_f32 * rows_f32, axis=1, keepdims=True)))


def norm_rows(rows_f32, totals, gain, bias, full_width):
    rows = rows_f32.shape[0]
    mean = totals[0:1, :] / full_width
    var = totals[1:2, :] / full_width - mean * mean
    rstd = lax.rsqrt(var + NORM_EPS)
    scaled = (rows_f32 - row_to_col(mean, rows)) * row_to_col(rstd, rows)
    return (scaled * gain + bias).astype(BF16)


def logits_kernel(
    cfg, hid_hbm, gain_hbm, bias_hbm, tok_hbm, egain_hbm, ebias_hbm, tab,
    z, lse, nin,
    hid, gain, bias, tok, egain, ebias, in_sem,
    hds_sem, hdr_sem, hxr_sem, extra, extra_sem,
    xn, out, xrecv, drecv, stg, tbuf, pick, ypick, runmax, runsum,
    ln_send, ln_recv, eln_send, eln_recv, fin_send, fin_recv,
    tab_sem, dsend_sem, drecv_sem, xsend_sem, xrecv_sem, ysend_sem, yrecv_sem,
    lns_sem, lnr_sem, els_sem, elr_sem, fis_sem, fir_sem,
):
    n, T, B, S, S2, n0, full_width, head, groups = cfg
    rows = hid.shape[0]
    dp = lax.axis_index("dp")
    v = lax.axis_index("vp")
    t = lax.axis_index("tp")
    x = lax.div(t, 2)
    c = lax.rem(t, 2)

    def peer(d):
        pv = 1 - v if d >= 4 else v
        px = 1 - x if (d // 2) % 2 else x
        pc = 1 - c if d % 2 else c
        return (dp, pv, 2 * px + pc)

    def start_table(j):
        a = lax.div(j, n)
        i = j - a * n
        xx = (1 - x) + a * (2 * x - 1)
        for w in range(2):
            cc = 1 - c if w == 0 else c
            row = pl.multiple_of((2 * xx + cc) * B + i * T, LANES)
            slot = lax.rem(j, S)
            pltpu.make_async_copy(tab.at[pl.ds(row, T)], tbuf.at[slot, w], tab_sem.at[slot]).start()

    def wait_table(j):
        slot = lax.rem(j, S)
        pltpu.make_async_copy(tbuf.at[slot], tbuf.at[slot], tab_sem.at[slot]).wait()

    def first_row(j, w):
        a = lax.div(j, n)
        i = j - a * n
        xx = (1 - x) + a * (2 * x - 1)
        cc = 1 - c if w == 0 else c
        return v * (4 * B) + (2 * xx + cc) * B + i * T

    def d2d_copy(j):
        slot = lax.rem(j, S2)
        return pltpu.make_async_remote_copy(
            src_ref=stg.at[slot], dst_ref=drecv.at[slot],
            send_sem=dsend_sem.at[slot], recv_sem=drecv_sem.at[slot],
            device_id=peer(1), device_id_type=MESH)

    def x_copy(g):
        first, last = groups[g]
        part = pl.ds(first, last - first)
        return pltpu.make_async_remote_copy(
            src_ref=out.at[part], dst_ref=xrecv.at[part],
            send_sem=xsend_sem, recv_sem=xrecv_sem.at[g],
            device_id=peer(2), device_id_type=MESH)

    def small_copy(src, dst, ssem, rsem, d):
        return pltpu.make_async_remote_copy(
            src_ref=src, dst_ref=dst.at[d - 1], send_sem=ssem, recv_sem=rsem,
            device_id=peer(d), device_id_type=MESH)

    def wait_small(dst, ssem, rsem):
        both = pltpu.make_async_remote_copy(
            src_ref=dst, dst_ref=dst, send_sem=ssem, recv_sem=rsem,
            device_id=peer(1), device_id_type=MESH)
        both.wait_recv()
        both.wait_send()

    barrier = pltpu.get_barrier_semaphore()
    for d in (4, 2, 3, 1):
        pl.semaphore_signal(barrier, inc=1, device_id=peer(d), device_id_type=MESH)

    pairs = ((hid_hbm, hid), (gain_hbm, gain), (bias_hbm, bias), (tok_hbm, tok),
             (egain_hbm, egain), (ebias_hbm, ebias))
    loads = [pltpu.make_async_copy(src, dst, in_sem.at[k]) for k, (src, dst) in enumerate(pairs)]
    for load in loads:
        load.start()
    for j in range(S):
        start_table(j)

    loads[0].wait()
    hid_f32 = hid[...].astype(F32)
    ln_send[...] = row_sums_tile(hid_f32)
    pl.semaphore_wait(barrier, 4)

    for d in (2, 3, 1):
        small_copy(ln_send, ln_recv, lns_sem, lnr_sem, d).start()
    for load in loads[1:]:
        load.wait()
    eye = (lax.broadcasted_iota(jnp.int32, (rows, rows), 0)
           == lax.broadcasted_iota(jnp.int32, (rows, rows), 1))
    tok_col = jnp.sum(
        jnp.where(eye, tok[...].astype(F32), 0.0), axis=1, keepdims=True).astype(jnp.int32)
    pick[...] = jnp.zeros_like(pick)
    runmax[...] = jnp.full(runmax.shape, -jnp.inf, F32)
    runsum[...] = jnp.zeros_like(runsum)
    wait_table(0)
    totals = ln_send[...]
    wait_small(ln_recv, lns_sem, lnr_sem)
    for d in range(3):
        totals = totals + ln_recv[d]
    xn[...] = norm_rows(hid_f32, totals, gain[...], bias[...], full_width)

    def matmul(j, w):
        slot = lax.rem(j, S)
        return lax.dot_general(
            xn[...], tbuf[slot, w], (((1,), (1,)), ((), ())), preferred_element_type=F32)

    def pick_rows(j):
        slot = lax.rem(j, S)
        total = pick[...]
        for w in range(2):
            local = tok_col - first_row(j, w)
            hot = (lax.broadcasted_iota(jnp.int32, (rows, T), 1) == local).astype(F32).astype(BF16)
            total = total + jnp.dot(hot, tbuf[slot, w], preferred_element_type=F32)
        pick[...] = total

    def zcols(i):
        return pl.ds(pl.multiple_of(i * T, LANES), T)

    def send_half(j):
        wait_table(j)

        @pl.when(j > S2)
        def _():
            d2d_copy(j - S2).wait_send()

        stg[lax.rem(j, S2)] = matmul(j, 0)

    def combine_out(i):
        d2d_copy(i).wait_recv()
        out[i] = out[i] + drecv[lax.rem(i, S2)]

    def refill(j):
        @pl.when(j + S < 2 * n)
        def _():
            start_table(j + S)

    def head_d2d(k):
        cols = pl.ds(head[k], head[k + 1] - head[k])
        return pltpu.make_async_remote_copy(
            src_ref=stg.at[0, :, cols], dst_ref=drecv.at[0, :, cols],
            send_sem=hds_sem, recv_sem=hdr_sem.at[k],
            device_id=peer(1), device_id_type=MESH)

    def head_x(k):
        cols = pl.ds(head[k], head[k + 1] - head[k])
        return pltpu.make_async_remote_copy(
            src_ref=out.at[0, :, cols], dst_ref=xrecv.at[0, :, cols],
            send_sem=xsend_sem, recv_sem=hxr_sem,
            device_id=peer(2), device_id_type=MESH)

    def head_matmul(k, w):
        return lax.dot_general(
            xn[...], tbuf[0, w, head[k]:head[k + 1], :], (((1,), (1,)), ((), ())),
            preferred_element_type=F32)

    def head_combine(k):
        head_d2d(k).wait_recv()
        cols = slice(head[k], head[k + 1])
        out[0, :, cols] = out[0, :, cols] + drecv[0, :, cols]

    pieces = len(head) - 1

    def head_give(k):
        stg[0, :, head[k]:head[k + 1]] = head_matmul(k, 0)

    def head_keep(k):
        out[0, :, head[k]:head[k + 1]] = head_matmul(k, 1)

    part_copy = pltpu.make_async_remote_copy(
        src_ref=stg.at[0, :, pl.ds(head[0], head[1])], dst_ref=extra,
        send_sem=hds_sem, recv_sem=extra_sem, device_id=peer(3), device_id_type=MESH)

    @pl.when(c == 0)
    def _():
        head_keep(0)
        head_keep(1)
        head_x(0).start()
        for k in range(2, pieces):
            head_keep(k)
        head_give(0)
        for k in range(1, pieces):
            head_combine(k)
            head_give(k)
            head_d2d(k - 1).start()
            head_x(k).start()
        head_d2d(pieces - 1).start()
        pick_rows(0)

    @pl.when(c == 1)
    def _():
        head_give(0)
        head_give(1)
        part_copy.start()
        for k in range(2, pieces):
            head_give(k)
            head_d2d(k - 1).start()
        head_keep(0)
        head_d2d(pieces - 1).start()
        for k in range(1, pieces):
            head_keep(k)
        pick_rows(0)
        for k in range(pieces):
            head_combine(k)

    refill(0)
    pltpu.make_async_remote_copy(
        src_ref=stg.at[0], dst_ref=drecv.at[0], send_sem=hds_sem, recv_sem=hdr_sem.at[0],
        device_id=peer(1), device_id_type=MESH).wait_send()

    @pl.loop(1, n)
    def _(j):
        @pl.when(j >= 2)
        def _():
            combine_out(j - 1)

        send_half(j)

        for g in range(n0):
            @pl.when(j == groups[g][1])
            def _():
                x_copy(g).start()

        d2d_copy(j).start()

        @pl.when(jnp.logical_and(c == 1, j == 1))
        def _():
            pltpu.make_async_remote_copy(
                src_ref=out.at[0], dst_ref=xrecv.at[0], send_sem=xsend_sem, recv_sem=hxr_sem,
                device_id=peer(2), device_id_type=MESH).start()

        out[j] = matmul(j, 1)
        pick_rows(j)
        refill(j)

    @pl.loop(n, 2 * n)
    def _(j):
        send_half(j)

        @pl.when(j == n)
        def _():
            combine_out(n - 1)

        @pl.when(j > n)
        def _():
            d2d_copy(j - 1).wait_recv()
            z[:, zcols(j - 1 - n)] = z[:, zcols(j - 1 - n)] + drecv[lax.rem(j - 1, S2)]

        d2d_copy(j).start()
        z[:, zcols(j - n)] = matmul(j, 1)
        pick_rows(j)
        refill(j)

    d2d_copy(2 * n - 1).wait_recv()
    z[:, zcols(n - 1)] = z[:, zcols(n - 1)] + drecv[(2 * n - 1) % S2]

    ycopy = pltpu.make_async_remote_copy(
        src_ref=pick, dst_ref=ypick, send_sem=ysend_sem, recv_sem=yrecv_sem,
        device_id=peer(4), device_id_type=MESH)
    ycopy.start()
    ycopy.wait()
    tok_rows = pick[...] + ypick[...]
    eln_send[...] = row_sums_tile(tok_rows)
    for d in range(1, 4):
        small_copy(eln_send, eln_recv, els_sem, elr_sem, d).start()
    for g in range(n0, len(groups)):
        x_copy(g).start()

    def absorb(i):
        m_old = runmax[...]
        m_new = m_old
        for k in range(T // LANES):
            cols = pl.ds(pl.multiple_of(i * T, LANES) + k * LANES, LANES)
            val = z[:, cols] + xrecv[i, :, k * LANES:(k + 1) * LANES]
            z[:, cols] = val
            m_new = jnp.maximum(m_new, val)
        s_new = runsum[...] * jnp.exp(m_old - m_new)
        for k in range(T // LANES):
            cols = pl.ds(pl.multiple_of(i * T, LANES) + k * LANES, LANES)
            s_new = s_new + jnp.exp(z[:, cols] - m_new)
        runmax[...] = m_new
        runsum[...] = s_new

    pltpu.make_async_remote_copy(
        src_ref=out.at[0], dst_ref=xrecv.at[0], send_sem=xsend_sem, recv_sem=hxr_sem,
        device_id=peer(2), device_id_type=MESH).wait_recv()

    @pl.when(c == 0)
    def _():
        part_copy.wait_recv()
        xrecv[0, :, head[0]:head[1]] = xrecv[0, :, head[0]:head[1]] + extra[...]

    absorb(0)
    for g, (first, last) in enumerate(groups):
        x_copy(g).wait_recv()

        @pl.loop(first, last)
        def _(i):
            absorb(i)

    top = jnp.max(runmax[...], axis=1, keepdims=True)
    exp_sum = jnp.sum(runsum[...] * jnp.exp(runmax[...] - top), axis=1, keepdims=True)
    fin_send[...] = two_rows(col_to_row(top), col_to_row(exp_sum))
    for d in (6, 7, 5, 4, 2, 3, 1):
        small_copy(fin_send, fin_recv, fis_sem, fir_sem, d).start()

    totals = eln_send[...]
    wait_small(eln_recv, els_sem, elr_sem)
    for d in range(3):
        totals = totals + eln_recv[d]
    nin[...] = norm_rows(pick[...] + ypick[...], totals, egain[...], ebias[...], full_width)

    pltpu.make_async_remote_copy(
        src_ref=out, dst_ref=xrecv, send_sem=xsend_sem, recv_sem=hxr_sem,
        device_id=peer(2), device_id_type=MESH).wait_send()

    @pl.loop(2 * n - S2, 2 * n)
    def _(j):
        d2d_copy(j).wait_send()

    tiles = [fin_send[...]]
    wait_small(fin_recv, fis_sem, fir_sem)
    for d in range(7):
        tiles.append(fin_recv[d])
    best = tiles[0][0:1, :]
    for tile in tiles[1:]:
        best = jnp.maximum(best, tile[0:1, :])
    total = jnp.zeros_like(best)
    for tile in tiles:
        total = total + tile[1:2, :] * jnp.exp(tile[0:1, :] - best)
    lse[...] = jnp.broadcast_to(best + jnp.log(total), lse.shape)


def finish_kernel(z, lse, nin, logp, log_sum, next_in, buf, row, sem, small_sem):
    rows, width = z.shape
    col = row_to_col(lse[0:1, :], rows)
    piece = 49 * LANES
    parts = [(r, lo, lo + piece) for r in range(0, rows, 8) for lo in range(0, width, piece)]

    def put(b):
        r, lo, hi = parts[b]
        part = (pl.ds(r, 8), pl.ds(lo, hi - lo))
        return pltpu.make_async_copy(buf.at[part], logp.at[part], sem)

    row[...] = lse[0:1, 0:rows]
    nin_copy = pltpu.make_async_copy(nin, next_in, small_sem.at[0])
    row_copy = pltpu.make_async_copy(row, log_sum, small_sem.at[1])
    for b, (r, lo, hi) in enumerate(parts):
        buf[r:r + 8, lo:hi] = z[r:r + 8, lo:hi] - col[r:r + 8, :]
        if b >= 1:
            put(b - 1).start(priority=b % 2)
        if b == 5:
            nin_copy.start()
            row_copy.start()
    put(len(parts) - 1).start()
    nin_copy.wait()
    row_copy.wait()
    pltpu.make_async_copy(buf, logp, sem).wait()


def solution(mesh):
    tp_size = mesh.shape["tp"]

    def per_device(hidden, lnf_gain, lnf_bias, emb_table, next_tok, eln_gain, eln_bias):
        rows, width = hidden.shape
        block = emb_table.shape[0] // tp_size
        T = 7 * LANES
        n = block // T
        S, S2, n0 = 3, 3, 5
        sizes = (1, 2, 5, 10, 10, 5, 1)
        groups, at = [], 1
        for size in sizes:
            groups.append((at, at + size))
            at += size
        head = (0, 3 * LANES, 5 * LANES, T)
        cfg = (n, T, block, S, S2, n0, float(width * tp_size), head, tuple(groups))
        vmem = pl.BlockSpec(memory_space=pltpu.VMEM)
        hbm = pl.BlockSpec(memory_space=pl.ANY)
        dma = pltpu.SemaphoreType.DMA
        z, lse, nin = pl.pallas_call(
            functools.partial(logits_kernel, cfg),
            out_shape=(
                pltpu.VMEM((rows, block), F32),
                pltpu.VMEM((8, LANES), F32),
                pltpu.VMEM((rows, width), BF16),
            ),
            in_specs=[hbm] * 7,
            out_specs=(vmem, vmem, vmem),
            scratch_shapes=[
                pltpu.VMEM((rows, width), BF16),
                pltpu.VMEM((1, width), F32),
                pltpu.VMEM((1, width), F32),
                pltpu.VMEM((1, rows), jnp.int32),
                pltpu.VMEM((1, width), F32),
                pltpu.VMEM((1, width), F32),
                dma((6,)),
                dma,
                dma((len(head) - 1,)),
                dma,
                pltpu.VMEM((rows, head[1]), F32),
                dma,
                pltpu.VMEM((rows, width), BF16),
                pltpu.VMEM((n, rows, T), F32),
                pltpu.VMEM((n, rows, T), F32),
                pltpu.VMEM((S2, rows, T), F32),
                pltpu.VMEM((S2, rows, T), F32),
                pltpu.VMEM((S, 2, T, width), BF16),
                pltpu.VMEM((rows, width), F32),
                pltpu.VMEM((rows, width), F32),
                pltpu.VMEM((rows, LANES), F32),
                pltpu.VMEM((rows, LANES), F32),
                pltpu.VMEM((8, LANES), F32),
                pltpu.VMEM((3, 8, LANES), F32),
                pltpu.VMEM((8, LANES), F32),
                pltpu.VMEM((3, 8, LANES), F32),
                pltpu.VMEM((8, LANES), F32),
                pltpu.VMEM((7, 8, LANES), F32),
                dma((S,)),
                dma((S2,)),
                dma((S2,)),
                dma,
                dma((len(groups),)),
                dma,
                dma,
                dma,
                dma,
                dma,
                dma,
                dma,
                dma,
            ],
            compiler_params=pltpu.CompilerParams(
                collective_id=0, has_side_effects=True, vmem_limit_bytes=52 * 2**20),
        )(hidden, lnf_gain.reshape(1, width), lnf_bias.reshape(1, width), next_tok.reshape(1, rows),
          eln_gain.reshape(1, width), eln_bias.reshape(1, width), emb_table)
        logp, log_sum, next_in = pl.pallas_call(
            finish_kernel,
            out_shape=(
                jax.ShapeDtypeStruct((rows, block), F32),
                jax.ShapeDtypeStruct((1, rows), F32),
                jax.ShapeDtypeStruct((rows, width), BF16),
            ),
            in_specs=[vmem, vmem, vmem],
            out_specs=(hbm, hbm, hbm),
            scratch_shapes=[
                pltpu.VMEM((rows, block), F32), pltpu.VMEM((1, rows), F32), dma, dma((2,))],
            compiler_params=pltpu.CompilerParams(vmem_limit_bytes=20 * 2**20),
        )(z, lse, nin)
        return logp, log_sum.reshape(rows), next_in

    return jax.shard_map(
        per_device,
        mesh=mesh,
        in_specs=(P("dp", "tp"), P("tp"), P("tp"), P("vp", "tp"), P("dp"), P("tp"), P("tp")),
        out_specs=(P("dp", ("vp", "tp")), P("dp"), P("dp", "tp")),
        check_vma=False,
    )
```

```python
import functools

import jax
import jax.numpy as jnp
from jax import lax
from jax.experimental import pallas as pl
from jax.experimental.pallas import tpu as pltpu
from jax.sharding import PartitionSpec as P

NORM_EPS = 1e-5
MESH = pl.DeviceIdType.MESH
F32 = jnp.float32
BF16 = jnp.bfloat16
LANES = 128


def diagonal(rows):
    return (lax.broadcasted_iota(jnp.int32, (rows, LANES), 0)
            == lax.broadcasted_iota(jnp.int32, (rows, LANES), 1))


def col_to_row(col):
    return jnp.sum(jnp.where(diagonal(col.shape[0]), col, jnp.zeros_like(col)), axis=0, keepdims=True)


def row_to_col(row, rows):
    return jnp.sum(jnp.where(diagonal(rows), row, jnp.zeros_like(row)), axis=1, keepdims=True)


def two_rows(first, second):
    sub = lax.broadcasted_iota(jnp.int32, (8, LANES), 0)
    return jnp.where(sub == 0, first, second)


def row_sums_tile(rows_f32):
    return two_rows(
        col_to_row(jnp.sum(rows_f32, axis=1, keepdims=True)),
        col_to_row(jnp.sum(rows_f32 * rows_f32, axis=1, keepdims=True)))


def norm_rows(rows_f32, totals, gain, bias, full_width):
    rows = rows_f32.shape[0]
    mean = totals[0:1, :] / full_width
    var = totals[1:2, :] / full_width - mean * mean
    rstd = lax.rsqrt(var + NORM_EPS)
    scaled = (rows_f32 - row_to_col(mean, rows)) * row_to_col(rstd, rows)
    return (scaled * gain + bias).astype(BF16)


def logits_kernel(
    cfg, hid_hbm, gain_hbm, bias_hbm, tok_hbm, egain_hbm, ebias_hbm, tab,
    z, lse, nin,
    hid, gain, bias, tok, egain, ebias, in_sem,
    hds_sem, hdr_sem, hxr_sem, extra, extra_sem,
    xn, out, xrecv, drecv, stg, tbuf, pick, ypick, runmax, runsum,
    ln_send, ln_recv, eln_send, eln_recv, fin_send, fin_recv,
    tab_sem, dsend_sem, drecv_sem, xsend_sem, xrecv_sem, yrecv_sem,
    lns_sem, lnr_sem, elr_sem, fis_sem, fir_sem,
):
    n, T, B, S, S2, n0, full_width, head, groups = cfg
    rows = hid.shape[0]
    dp = lax.axis_index("dp")
    v = lax.axis_index("vp")
    t = lax.axis_index("tp")
    x = lax.div(t, 2)
    c = lax.rem(t, 2)

    def peer(d):
        pv = 1 - v if d >= 4 else v
        px = 1 - x if (d // 2) % 2 else x
        pc = 1 - c if d % 2 else c
        return (dp, pv, 2 * px + pc)

    def start_table(j):
        a = lax.div(j, n)
        i = j - a * n
        xx = (1 - x) + a * (2 * x - 1)
        for w in range(2):
            cc = 1 - c if w == 0 else c
            row = pl.multiple_of((2 * xx + cc) * B + i * T, LANES)
            slot = lax.rem(j, S)
            pltpu.make_async_copy(tab.at[pl.ds(row, T)], tbuf.at[slot, w], tab_sem.at[slot]).start()

    def wait_table(j):
        slot = lax.rem(j, S)
        pltpu.make_async_copy(tbuf.at[slot], tbuf.at[slot], tab_sem.at[slot]).wait()

    def first_row(j, w):
        a = lax.div(j, n)
        i = j - a * n
        xx = (1 - x) + a * (2 * x - 1)
        cc = 1 - c if w == 0 else c
        return v * (4 * B) + (2 * xx + cc) * B + i * T

    def d2d_copy(j):
        slot = lax.rem(j, S2)
        return pltpu.make_async_remote_copy(
            src_ref=stg.at[slot], dst_ref=drecv.at[slot],
            send_sem=dsend_sem.at[slot], recv_sem=drecv_sem.at[slot],
            device_id=peer(1), device_id_type=MESH)

    def x_copy(g):
        first, last = groups[g]
        part = pl.ds(first, last - first)
        return pltpu.make_async_remote_copy(
            src_ref=out.at[part], dst_ref=xrecv.at[part],
            send_sem=xsend_sem, recv_sem=xrecv_sem.at[g],
            device_id=peer(2), device_id_type=MESH)

    def small_copy(src, dst, ssem, rsem, d):
        return pltpu.make_async_remote_copy(
            src_ref=src, dst_ref=dst.at[d - 1], send_sem=ssem, recv_sem=rsem,
            device_id=peer(d), device_id_type=MESH)

    def wait_small(dst, ssem, rsem):
        both = pltpu.make_async_remote_copy(
            src_ref=dst, dst_ref=dst, send_sem=ssem, recv_sem=rsem,
            device_id=peer(1), device_id_type=MESH)
        both.wait_recv()
        both.wait_send()

    barrier = pltpu.get_barrier_semaphore()
    for d in (4, 2, 3, 1):
        pl.semaphore_signal(barrier, inc=1, device_id=peer(d), device_id_type=MESH)

    pairs = ((hid_hbm, hid), (gain_hbm, gain), (bias_hbm, bias), (tok_hbm, tok),
             (egain_hbm, egain), (ebias_hbm, ebias))
    loads = [pltpu.make_async_copy(src, dst, in_sem.at[slot]) for slot, (src, dst) in zip((0, 1, 1, 2, 1, 1), pairs)]
    for load in loads:
        load.start()
    for j in range(S):
        start_table(j)

    loads[0].wait()
    hid_f32 = hid[...].astype(F32)
    ln_send[...] = row_sums_tile(hid_f32)
    pl.semaphore_wait(barrier, 4)

    for d in (2, 3, 1):
        small_copy(ln_send, ln_recv, lns_sem, lnr_sem, d).start()
    loads[3].wait()
    four = fin_recv.at[pl.ds(0, 2)]
    pltpu.make_async_copy(four, four, in_sem.at[1]).wait()
    eye = (lax.broadcasted_iota(jnp.int32, (rows, rows), 0)
           == lax.broadcasted_iota(jnp.int32, (rows, rows), 1))
    tok_col = jnp.sum(
        jnp.where(eye, tok[...].astype(F32), 0.0), axis=1, keepdims=True).astype(jnp.int32)
    pick[...] = jnp.zeros_like(pick)
    runmax[...] = jnp.full(runmax.shape, -jnp.inf, F32)
    runsum[...] = jnp.zeros_like(runsum)
    wait_table(0)
    totals = ln_send[...]
    wait_small(ln_recv, lns_sem, lnr_sem)
    for d in range(3):
        totals = totals + ln_recv[d]
    xn[...] = norm_rows(hid_f32, totals, gain[...], bias[...], full_width)

    def matmul(j, w):
        slot = lax.rem(j, S)
        return lax.dot_general(
            xn[...], tbuf[slot, w], (((1,), (1,)), ((), ())), preferred_element_type=F32)

    def pick_rows(j):
        slot = lax.rem(j, S)
        total = pick[...]
        for w in range(2):
            local = tok_col - first_row(j, w)
            hot = (lax.broadcasted_iota(jnp.int32, (rows, T), 1) == local).astype(F32).astype(BF16)
            total = total + jnp.dot(hot, tbuf[slot, w], preferred_element_type=F32)
        pick[...] = total

    def zcols(i):
        return pl.ds(pl.multiple_of(i * T, LANES), T)

    def send_half(j):
        wait_table(j)

        @pl.when(j > S2)
        def _():
            d2d_copy(j - S2).wait_send()

        stg[lax.rem(j, S2)] = matmul(j, 0)

    def combine_out(i):
        d2d_copy(i).wait_recv()
        out[i] = out[i] + drecv[lax.rem(i, S2)]

    def refill(j):
        @pl.when(j + S < 2 * n)
        def _():
            start_table(j + S)

    def head_d2d(k):
        cols = pl.ds(head[k], head[k + 1] - head[k])
        return pltpu.make_async_remote_copy(
            src_ref=stg.at[0, :, cols], dst_ref=drecv.at[0, :, cols],
            send_sem=hds_sem, recv_sem=hdr_sem.at[k],
            device_id=peer(1), device_id_type=MESH)

    def head_x(k):
        cols = pl.ds(head[k], head[k + 1] - head[k])
        return pltpu.make_async_remote_copy(
            src_ref=out.at[0, :, cols], dst_ref=xrecv.at[0, :, cols],
            send_sem=xsend_sem, recv_sem=hxr_sem,
            device_id=peer(2), device_id_type=MESH)

    def head_matmul(k, w):
        return lax.dot_general(
            xn[...], tbuf[0, w, head[k]:head[k + 1], :], (((1,), (1,)), ((), ())),
            preferred_element_type=F32)

    def head_combine(k):
        head_d2d(k).wait_recv()
        cols = slice(head[k], head[k + 1])
        out[0, :, cols] = out[0, :, cols] + drecv[0, :, cols]

    pieces = len(head) - 1

    def head_give(k):
        stg[0, :, head[k]:head[k + 1]] = head_matmul(k, 0)

    def head_keep(k):
        out[0, :, head[k]:head[k + 1]] = head_matmul(k, 1)

    part_copy = pltpu.make_async_remote_copy(
        src_ref=stg.at[0, :, pl.ds(head[0], head[1])], dst_ref=extra,
        send_sem=hds_sem, recv_sem=extra_sem, device_id=peer(3), device_id_type=MESH)

    @pl.when(c == 0)
    def _():
        head_keep(0)
        head_keep(1)
        head_x(0).start()
        for k in range(2, pieces):
            head_keep(k)
        head_give(0)
        for k in range(1, pieces):
            head_combine(k)
            head_give(k)
            head_d2d(k - 1).start()
            head_x(k).start()
        head_d2d(pieces - 1).start()
        pick_rows(0)

    @pl.when(c == 1)
    def _():
        head_give(0)
        head_give(1)
        part_copy.start()
        for k in range(2, pieces):
            head_give(k)
            head_d2d(k - 1).start()
        head_keep(0)
        head_d2d(pieces - 1).start()
        for k in range(1, pieces):
            head_keep(k)
        pick_rows(0)
        for k in range(pieces):
            head_combine(k)

    refill(0)
    pltpu.make_async_remote_copy(
        src_ref=stg.at[0], dst_ref=drecv.at[0], send_sem=hds_sem, recv_sem=hdr_sem.at[0],
        device_id=peer(1), device_id_type=MESH).wait_send()

    @pl.loop(1, n)
    def _(j):
        @pl.when(j >= 2)
        def _():
            combine_out(j - 1)

        send_half(j)

        for g in range(n0):
            @pl.when(j == groups[g][1])
            def _():
                x_copy(g).start()

        d2d_copy(j).start()

        @pl.when(jnp.logical_and(c == 1, j == 1))
        def _():
            pltpu.make_async_remote_copy(
                src_ref=out.at[0], dst_ref=xrecv.at[0], send_sem=xsend_sem, recv_sem=hxr_sem,
                device_id=peer(2), device_id_type=MESH).start()

        out[j] = matmul(j, 1)
        pick_rows(j)
        refill(j)

    @pl.loop(n, 2 * n)
    def _(j):
        send_half(j)

        @pl.when(j == n)
        def _():
            combine_out(n - 1)

        @pl.when(j > n)
        def _():
            d2d_copy(j - 1).wait_recv()
            z[:, zcols(j - 1 - n)] = z[:, zcols(j - 1 - n)] + drecv[lax.rem(j - 1, S2)]

        d2d_copy(j).start()
        z[:, zcols(j - n)] = matmul(j, 1)
        pick_rows(j)
        refill(j)

    d2d_copy(2 * n - 1).wait_recv()
    z[:, zcols(n - 1)] = z[:, zcols(n - 1)] + drecv[(2 * n - 1) % S2]

    ycopy = pltpu.make_async_remote_copy(
        src_ref=pick, dst_ref=ypick, send_sem=hds_sem, recv_sem=yrecv_sem,
        device_id=peer(4), device_id_type=MESH)
    ycopy.start()
    ycopy.wait()
    tok_rows = pick[...] + ypick[...]
    eln_send[...] = row_sums_tile(tok_rows)
    for d in range(1, 4):
        small_copy(eln_send, eln_recv, lns_sem, elr_sem, d).start()
    for g in range(n0, len(groups)):
        x_copy(g).start()

    def absorb(i):
        m_old = runmax[...]
        m_new = m_old
        for k in range(T // LANES):
            cols = pl.ds(pl.multiple_of(i * T, LANES) + k * LANES, LANES)
            val = z[:, cols] + xrecv[i, :, k * LANES:(k + 1) * LANES]
            z[:, cols] = val
            m_new = jnp.maximum(m_new, val)
        s_new = runsum[...] * jnp.exp(m_old - m_new)
        for k in range(T // LANES):
            cols = pl.ds(pl.multiple_of(i * T, LANES) + k * LANES, LANES)
            s_new = s_new + jnp.exp(z[:, cols] - m_new)
        runmax[...] = m_new
        runsum[...] = s_new

    pltpu.make_async_remote_copy(
        src_ref=out.at[0], dst_ref=xrecv.at[0], send_sem=xsend_sem, recv_sem=hxr_sem,
        device_id=peer(2), device_id_type=MESH).wait_recv()

    @pl.when(c == 0)
    def _():
        part_copy.wait_recv()
        xrecv[0, :, head[0]:head[1]] = xrecv[0, :, head[0]:head[1]] + extra[...]

    absorb(0)
    for g, (first, last) in enumerate(groups):
        x_copy(g).wait_recv()

        @pl.loop(first, last)
        def _(i):
            absorb(i)

    top = jnp.max(runmax[...], axis=1, keepdims=True)
    exp_sum = jnp.sum(runsum[...] * jnp.exp(runmax[...] - top), axis=1, keepdims=True)
    fin_send[...] = two_rows(col_to_row(top), col_to_row(exp_sum))
    for d in (6, 7, 5, 4, 2, 3, 1):
        small_copy(fin_send, fin_recv, fis_sem, fir_sem, d).start()

    totals = eln_send[...]
    wait_small(eln_recv, lns_sem, elr_sem)
    for d in range(3):
        totals = totals + eln_recv[d]
    nin[...] = norm_rows(pick[...] + ypick[...], totals, egain[...], ebias[...], full_width)

    pltpu.make_async_remote_copy(
        src_ref=out, dst_ref=xrecv, send_sem=xsend_sem, recv_sem=hxr_sem,
        device_id=peer(2), device_id_type=MESH).wait_send()

    @pl.loop(2 * n - S2, 2 * n)
    def _(j):
        d2d_copy(j).wait_send()

    tiles = [fin_send[...]]
    wait_small(fin_recv, fis_sem, fir_sem)
    for d in range(7):
        tiles.append(fin_recv[d])
    best = tiles[0][0:1, :]
    for tile in tiles[1:]:
        best = jnp.maximum(best, tile[0:1, :])
    total = jnp.zeros_like(best)
    for tile in tiles:
        total = total + tile[1:2, :] * jnp.exp(tile[0:1, :] - best)
    lse[...] = jnp.broadcast_to(best + jnp.log(total), lse.shape)


def finish_kernel(z, lse, nin, logp, log_sum, next_in, buf, row, sem, small_sem):
    rows, width = z.shape
    col = row_to_col(lse[0:1, :], rows)
    piece = 49 * LANES
    parts = [(r, lo, lo + piece) for r in range(0, rows, 8) for lo in range(0, width, piece)]

    def put(b):
        r, lo, hi = parts[b]
        part = (pl.ds(r, 8), pl.ds(lo, hi - lo))
        return pltpu.make_async_copy(buf.at[part], logp.at[part], sem)

    row[...] = lse[0:1, 0:rows]
    nin_copy = pltpu.make_async_copy(nin, next_in, small_sem.at[0])
    row_copy = pltpu.make_async_copy(row, log_sum, small_sem.at[1])
    for b, (r, lo, hi) in enumerate(parts):
        buf[r:r + 8, lo:hi] = z[r:r + 8, lo:hi] - col[r:r + 8, :]
        if b >= 1:
            put(b - 1).start(priority=b % 2)
        if b == 5:
            nin_copy.start()
            row_copy.start()
    put(len(parts) - 1).start()
    nin_copy.wait()
    row_copy.wait()
    pltpu.make_async_copy(buf, logp, sem).wait()


def solution(mesh):
    tp_size = mesh.shape["tp"]

    def per_device(hidden, lnf_gain, lnf_bias, emb_table, next_tok, eln_gain, eln_bias):
        rows, width = hidden.shape
        block = emb_table.shape[0] // tp_size
        T = 7 * LANES
        n = block // T
        S, S2, n0 = 3, 3, 5
        sizes = (1, 2, 5, 10, 10, 5, 1)
        groups, at = [], 1
        for size in sizes:
            groups.append((at, at + size))
            at += size
        head = (0, 3 * LANES, 5 * LANES, T)
        cfg = (n, T, block, S, S2, n0, float(width * tp_size), head, tuple(groups))
        vmem = pl.BlockSpec(memory_space=pltpu.VMEM)
        hbm = pl.BlockSpec(memory_space=pl.ANY)
        dma = pltpu.SemaphoreType.DMA
        z, lse, nin = pl.pallas_call(
            functools.partial(logits_kernel, cfg),
            out_shape=(
                pltpu.VMEM((rows, block), F32),
                pltpu.VMEM((8, LANES), F32),
                pltpu.VMEM((rows, width), BF16),
            ),
            in_specs=[hbm] * 7,
            out_specs=(vmem, vmem, vmem),
            scratch_shapes=[
                pltpu.VMEM((rows, width), BF16),
                pltpu.VMEM((1, width), F32),
                pltpu.VMEM((1, width), F32),
                pltpu.VMEM((1, rows), jnp.int32),
                pltpu.VMEM((1, width), F32),
                pltpu.VMEM((1, width), F32),
                dma((3,)),
                dma,
                dma((len(head) - 1,)),
                dma,
                pltpu.VMEM((rows, head[1]), F32),
                dma,
                pltpu.VMEM((rows, width), BF16),
                pltpu.VMEM((n, rows, T), F32),
                pltpu.VMEM((n, rows, T), F32),
                pltpu.VMEM((S2, rows, T), F32),
                pltpu.VMEM((S2, rows, T), F32),
                pltpu.VMEM((S, 2, T, width), BF16),
                pltpu.VMEM((rows, width), F32),
                pltpu.VMEM((rows, width), F32),
                pltpu.VMEM((rows, LANES), F32),
                pltpu.VMEM((rows, LANES), F32),
                pltpu.VMEM((8, LANES), F32),
                pltpu.VMEM((3, 8, LANES), F32),
                pltpu.VMEM((8, LANES), F32),
                pltpu.VMEM((3, 8, LANES), F32),
                pltpu.VMEM((8, LANES), F32),
                pltpu.VMEM((7, 8, LANES), F32),
                dma((S,)),
                dma((S2,)),
                dma((S2,)),
                dma,
                dma((len(groups),)),
                dma,
                dma,
                dma,
                dma,
                dma,
                dma,
            ],
            compiler_params=pltpu.CompilerParams(
                collective_id=0, has_side_effects=True, vmem_limit_bytes=52 * 2**20),
        )(hidden, lnf_gain.reshape(1, width), lnf_bias.reshape(1, width), next_tok.reshape(1, rows),
          eln_gain.reshape(1, width), eln_bias.reshape(1, width), emb_table)
        logp, log_sum, next_in = pl.pallas_call(
            finish_kernel,
            out_shape=(
                jax.ShapeDtypeStruct((rows, block), F32),
                jax.ShapeDtypeStruct((1, rows), F32),
                jax.ShapeDtypeStruct((rows, width), BF16),
            ),
            in_specs=[vmem, vmem, vmem],
            out_specs=(hbm, hbm, hbm),
            scratch_shapes=[
                pltpu.VMEM((rows, block), F32), pltpu.VMEM((1, rows), F32), dma, dma((2,))],
            compiler_params=pltpu.CompilerParams(vmem_limit_bytes=20 * 2**20),
        )(z, lse, nin)
        return logp, log_sum.reshape(rows), next_in

    return jax.shard_map(
        per_device,
        mesh=mesh,
        in_specs=(P("dp", "tp"), P("tp"), P("tp"), P("vp", "tp"), P("dp"), P("tp"), P("tp")),
        out_specs=(P("dp", ("vp", "tp")), P("dp"), P("dp", "tp")),
        check_vma=False,
    )
```

```python
import functools

import jax
import jax.numpy as jnp
from jax import lax
from jax.experimental import pallas as pl
from jax.experimental.pallas import tpu as pltpu
from jax.sharding import PartitionSpec as P

NORM_EPS = 1e-5
MESH = pl.DeviceIdType.MESH
F32 = jnp.float32
BF16 = jnp.bfloat16
LANES = 128


def diagonal(rows):
    return (lax.broadcasted_iota(jnp.int32, (rows, LANES), 0)
            == lax.broadcasted_iota(jnp.int32, (rows, LANES), 1))


def col_to_row(col):
    return jnp.sum(jnp.where(diagonal(col.shape[0]), col, jnp.zeros_like(col)), axis=0, keepdims=True)


def row_to_col(row, rows):
    return jnp.sum(jnp.where(diagonal(rows), row, jnp.zeros_like(row)), axis=1, keepdims=True)


def two_rows(first, second):
    sub = lax.broadcasted_iota(jnp.int32, (8, LANES), 0)
    return jnp.where(sub == 0, first, second)


def row_sums_tile(rows_f32):
    return two_rows(
        col_to_row(jnp.sum(rows_f32, axis=1, keepdims=True)),
        col_to_row(jnp.sum(rows_f32 * rows_f32, axis=1, keepdims=True)))


def norm_rows(rows_f32, totals, gain, bias, full_width):
    rows = rows_f32.shape[0]
    mean = totals[0:1, :] / full_width
    var = totals[1:2, :] / full_width - mean * mean
    rstd = lax.rsqrt(var + NORM_EPS)
    scaled = (rows_f32 - row_to_col(mean, rows)) * row_to_col(rstd, rows)
    return (scaled * gain + bias).astype(BF16)


def logits_kernel(
    cfg, hid_hbm, gain_hbm, bias_hbm, tok_hbm, egain_hbm, ebias_hbm, tab,
    z, lse, nin,
    hid, gain, bias, tok, egain, ebias, in_sem,
    hds_sem, hdr_sem, hxr_sem, extra, extra_sem,
    xn, out, xrecv, drecv, stg, tbuf, pick, ypick, runmax, runsum,
    ln_send, ln_recv, eln_send, eln_recv, fin_send, fin_recv,
    tab_sem, dsend_sem, drecv_sem, xsend_sem, xrecv_sem, yrecv_sem,
    lns_sem, lnr_sem, elr_sem, fir_sem,
):
    n, T, B, S, S2, n0, full_width, head, groups = cfg
    rows = hid.shape[0]
    dp = lax.axis_index("dp")
    v = lax.axis_index("vp")
    t = lax.axis_index("tp")
    x = lax.div(t, 2)
    c = lax.rem(t, 2)

    def peer(d):
        pv = 1 - v if d >= 4 else v
        px = 1 - x if (d // 2) % 2 else x
        pc = 1 - c if d % 2 else c
        return (dp, pv, 2 * px + pc)

    def start_table(j):
        a = lax.div(j, n)
        i = j - a * n
        xx = (1 - x) + a * (2 * x - 1)
        for w in range(2):
            cc = 1 - c if w == 0 else c
            row = pl.multiple_of((2 * xx + cc) * B + i * T, LANES)
            slot = lax.rem(j, S)
            pltpu.make_async_copy(tab.at[pl.ds(row, T)], tbuf.at[slot, w], tab_sem.at[slot]).start()

    def wait_table(j):
        slot = lax.rem(j, S)
        pltpu.make_async_copy(tbuf.at[slot], tbuf.at[slot], tab_sem.at[slot]).wait()

    def first_row(j, w):
        a = lax.div(j, n)
        i = j - a * n
        xx = (1 - x) + a * (2 * x - 1)
        cc = 1 - c if w == 0 else c
        return v * (4 * B) + (2 * xx + cc) * B + i * T

    def d2d_copy(j):
        slot = lax.rem(j, S2)
        return pltpu.make_async_remote_copy(
            src_ref=stg.at[slot], dst_ref=drecv.at[slot],
            send_sem=dsend_sem.at[slot], recv_sem=drecv_sem.at[slot],
            device_id=peer(1), device_id_type=MESH)

    def x_copy(g):
        first, last = groups[g]
        part = pl.ds(first, last - first)
        return pltpu.make_async_remote_copy(
            src_ref=out.at[part], dst_ref=xrecv.at[part],
            send_sem=xsend_sem, recv_sem=xrecv_sem.at[g],
            device_id=peer(2), device_id_type=MESH)

    def small_copy(src, dst, ssem, rsem, d):
        return pltpu.make_async_remote_copy(
            src_ref=src, dst_ref=dst.at[d - 1], send_sem=ssem, recv_sem=rsem,
            device_id=peer(d), device_id_type=MESH)

    def wait_small(dst, ssem, rsem):
        both = pltpu.make_async_remote_copy(
            src_ref=dst, dst_ref=dst, send_sem=ssem, recv_sem=rsem,
            device_id=peer(1), device_id_type=MESH)
        both.wait_recv()
        both.wait_send()

    barrier = pltpu.get_barrier_semaphore()
    for d in (4, 2, 3, 1):
        pl.semaphore_signal(barrier, inc=1, device_id=peer(d), device_id_type=MESH)

    pairs = ((hid_hbm, hid), (gain_hbm, gain), (bias_hbm, bias), (tok_hbm, tok),
             (egain_hbm, egain), (ebias_hbm, ebias))
    loads = [pltpu.make_async_copy(src, dst, in_sem.at[slot]) for slot, (src, dst) in zip((0, 1, 1, 2, 1, 1), pairs)]
    for load in loads:
        load.start()
    for j in range(S):
        start_table(j)

    loads[0].wait()
    hid_f32 = hid[...].astype(F32)
    ln_send[...] = row_sums_tile(hid_f32)
    pl.semaphore_wait(barrier, 4)

    for d in (2, 3, 1):
        small_copy(ln_send, ln_recv, lns_sem, lnr_sem, d).start()
    loads[3].wait()
    four = fin_recv.at[pl.ds(0, 2)]
    pltpu.make_async_copy(four, four, in_sem.at[1]).wait()
    eye = (lax.broadcasted_iota(jnp.int32, (rows, rows), 0)
           == lax.broadcasted_iota(jnp.int32, (rows, rows), 1))
    tok_col = jnp.sum(
        jnp.where(eye, tok[...].astype(F32), 0.0), axis=1, keepdims=True).astype(jnp.int32)
    pick[...] = jnp.zeros_like(pick)
    runmax[...] = jnp.full(runmax.shape, -jnp.inf, F32)
    runsum[...] = jnp.zeros_like(runsum)
    wait_table(0)
    totals = ln_send[...]
    wait_small(ln_recv, lns_sem, lnr_sem)
    for d in range(3):
        totals = totals + ln_recv[d]
    xn[...] = norm_rows(hid_f32, totals, gain[...], bias[...], full_width)

    def matmul(j, w):
        slot = lax.rem(j, S)
        return lax.dot_general(
            xn[...], tbuf[slot, w], (((1,), (1,)), ((), ())), preferred_element_type=F32)

    def pick_rows(j):
        slot = lax.rem(j, S)
        total = pick[...]
        for w in range(2):
            local = tok_col - first_row(j, w)
            hot = (lax.broadcasted_iota(jnp.int32, (rows, T), 1) == local).astype(F32).astype(BF16)
            total = total + jnp.dot(hot, tbuf[slot, w], preferred_element_type=F32)
        pick[...] = total

    def zcols(i):
        return pl.ds(pl.multiple_of(i * T, LANES), T)

    def send_half(j):
        wait_table(j)

        @pl.when(j > S2)
        def _():
            d2d_copy(j - S2).wait_send()

        stg[lax.rem(j, S2)] = matmul(j, 0)

    def combine_out(i):
        d2d_copy(i).wait_recv()
        out[i] = out[i] + drecv[lax.rem(i, S2)]

    def refill(j):
        @pl.when(j + S < 2 * n)
        def _():
            start_table(j + S)

    def head_d2d(k):
        cols = pl.ds(head[k], head[k + 1] - head[k])
        return pltpu.make_async_remote_copy(
            src_ref=stg.at[0, :, cols], dst_ref=drecv.at[0, :, cols],
            send_sem=hds_sem, recv_sem=hdr_sem.at[k],
            device_id=peer(1), device_id_type=MESH)

    def head_x(k):
        cols = pl.ds(head[k], head[k + 1] - head[k])
        return pltpu.make_async_remote_copy(
            src_ref=out.at[0, :, cols], dst_ref=xrecv.at[0, :, cols],
            send_sem=xsend_sem, recv_sem=hxr_sem,
            device_id=peer(2), device_id_type=MESH)

    def head_matmul(k, w):
        return lax.dot_general(
            xn[...], tbuf[0, w, head[k]:head[k + 1], :], (((1,), (1,)), ((), ())),
            preferred_element_type=F32)

    def head_combine(k):
        head_d2d(k).wait_recv()
        cols = slice(head[k], head[k + 1])
        out[0, :, cols] = out[0, :, cols] + drecv[0, :, cols]

    pieces = len(head) - 1

    def head_give(k):
        stg[0, :, head[k]:head[k + 1]] = head_matmul(k, 0)

    def head_keep(k):
        out[0, :, head[k]:head[k + 1]] = head_matmul(k, 1)

    part_copy = pltpu.make_async_remote_copy(
        src_ref=stg.at[0, :, pl.ds(head[0], head[1])], dst_ref=extra,
        send_sem=hds_sem, recv_sem=extra_sem, device_id=peer(3), device_id_type=MESH)

    @pl.when(c == 0)
    def _():
        head_keep(0)
        head_keep(1)
        head_x(0).start()
        for k in range(2, pieces):
            head_keep(k)
        head_give(0)
        for k in range(1, pieces):
            head_combine(k)
            head_give(k)
            head_d2d(k - 1).start()
            head_x(k).start()
        head_d2d(pieces - 1).start()
        pick_rows(0)

    @pl.when(c == 1)
    def _():
        head_give(0)
        head_give(1)
        part_copy.start()
        for k in range(2, pieces):
            head_give(k)
            head_d2d(k - 1).start()
        head_keep(0)
        head_d2d(pieces - 1).start()
        for k in range(1, pieces):
            head_keep(k)
        pick_rows(0)
        for k in range(pieces):
            head_combine(k)

    refill(0)
    pltpu.make_async_remote_copy(
        src_ref=stg.at[0], dst_ref=drecv.at[0], send_sem=hds_sem, recv_sem=hdr_sem.at[0],
        device_id=peer(1), device_id_type=MESH).wait_send()

    @pl.loop(1, n)
    def _(j):
        @pl.when(j >= 2)
        def _():
            combine_out(j - 1)

        send_half(j)

        for g in range(n0):
            @pl.when(j == groups[g][1])
            def _():
                x_copy(g).start()

        d2d_copy(j).start()

        @pl.when(jnp.logical_and(c == 1, j == 1))
        def _():
            pltpu.make_async_remote_copy(
                src_ref=out.at[0], dst_ref=xrecv.at[0], send_sem=xsend_sem, recv_sem=hxr_sem,
                device_id=peer(2), device_id_type=MESH).start()

        out[j] = matmul(j, 1)
        pick_rows(j)
        refill(j)

    @pl.loop(n, 2 * n)
    def _(j):
        send_half(j)

        @pl.when(j == n)
        def _():
            combine_out(n - 1)

        @pl.when(j > n)
        def _():
            d2d_copy(j - 1).wait_recv()
            z[:, zcols(j - 1 - n)] = z[:, zcols(j - 1 - n)] + drecv[lax.rem(j - 1, S2)]

        d2d_copy(j).start()
        z[:, zcols(j - n)] = matmul(j, 1)
        pick_rows(j)
        refill(j)

    d2d_copy(2 * n - 1).wait_recv()
    z[:, zcols(n - 1)] = z[:, zcols(n - 1)] + drecv[(2 * n - 1) % S2]

    ycopy = pltpu.make_async_remote_copy(
        src_ref=pick, dst_ref=ypick, send_sem=hds_sem, recv_sem=yrecv_sem,
        device_id=peer(4), device_id_type=MESH)
    ycopy.start()
    ycopy.wait()
    tok_rows = pick[...] + ypick[...]
    eln_send[...] = row_sums_tile(tok_rows)
    for d in range(1, 4):
        small_copy(eln_send, eln_recv, lns_sem, elr_sem, d).start()
    for g in range(n0, len(groups)):
        x_copy(g).start()

    def absorb(i):
        m_old = runmax[...]
        m_new = m_old
        for k in range(T // LANES):
            cols = pl.ds(pl.multiple_of(i * T, LANES) + k * LANES, LANES)
            val = z[:, cols] + xrecv[i, :, k * LANES:(k + 1) * LANES]
            z[:, cols] = val
            m_new = jnp.maximum(m_new, val)
        s_new = runsum[...] * jnp.exp(m_old - m_new)
        for k in range(T // LANES):
            cols = pl.ds(pl.multiple_of(i * T, LANES) + k * LANES, LANES)
            s_new = s_new + jnp.exp(z[:, cols] - m_new)
        runmax[...] = m_new
        runsum[...] = s_new

    pltpu.make_async_remote_copy(
        src_ref=out.at[0], dst_ref=xrecv.at[0], send_sem=xsend_sem, recv_sem=hxr_sem,
        device_id=peer(2), device_id_type=MESH).wait_recv()

    @pl.when(c == 0)
    def _():
        part_copy.wait_recv()
        xrecv[0, :, head[0]:head[1]] = xrecv[0, :, head[0]:head[1]] + extra[...]

    absorb(0)
    for g, (first, last) in enumerate(groups):
        x_copy(g).wait_recv()

        @pl.loop(first, last)
        def _(i):
            absorb(i)

    top = jnp.max(runmax[...], axis=1, keepdims=True)
    exp_sum = jnp.sum(runsum[...] * jnp.exp(runmax[...] - top), axis=1, keepdims=True)
    fin_send[...] = two_rows(col_to_row(top), col_to_row(exp_sum))
    for d in (6, 7, 5, 4, 2, 3, 1):
        small_copy(fin_send, fin_recv, hds_sem, fir_sem, d).start()

    totals = eln_send[...]
    wait_small(eln_recv, lns_sem, elr_sem)
    for d in range(3):
        totals = totals + eln_recv[d]
    nin[...] = norm_rows(pick[...] + ypick[...], totals, egain[...], ebias[...], full_width)

    pltpu.make_async_remote_copy(
        src_ref=out, dst_ref=xrecv, send_sem=xsend_sem, recv_sem=hxr_sem,
        device_id=peer(2), device_id_type=MESH).wait_send()

    @pl.loop(2 * n - S2, 2 * n)
    def _(j):
        d2d_copy(j).wait_send()

    tiles = [fin_send[...]]
    wait_small(fin_recv, hds_sem, fir_sem)
    for d in range(7):
        tiles.append(fin_recv[d])
    best = tiles[0][0:1, :]
    for tile in tiles[1:]:
        best = jnp.maximum(best, tile[0:1, :])
    total = jnp.zeros_like(best)
    for tile in tiles:
        total = total + tile[1:2, :] * jnp.exp(tile[0:1, :] - best)
    lse[...] = jnp.broadcast_to(best + jnp.log(total), lse.shape)


def finish_kernel(z, lse, nin, logp, log_sum, next_in, buf, row, sem, small_sem):
    rows, width = z.shape
    col = row_to_col(lse[0:1, :], rows)
    piece = 49 * LANES
    parts = [(r, lo, lo + piece) for r in range(0, rows, 8) for lo in range(0, width, piece)]

    def put(b):
        r, lo, hi = parts[b]
        part = (pl.ds(r, 8), pl.ds(lo, hi - lo))
        return pltpu.make_async_copy(buf.at[part], logp.at[part], sem)

    row[...] = lse[0:1, 0:rows]
    nin_copy = pltpu.make_async_copy(nin, next_in, small_sem.at[0])
    row_copy = pltpu.make_async_copy(row, log_sum, small_sem.at[1])
    for b, (r, lo, hi) in enumerate(parts):
        buf[r:r + 8, lo:hi] = z[r:r + 8, lo:hi] - col[r:r + 8, :]
        if b >= 1:
            put(b - 1).start(priority=b % 2)
        if b == 5:
            nin_copy.start()
            row_copy.start()
    put(len(parts) - 1).start()
    nin_copy.wait()
    row_copy.wait()
    pltpu.make_async_copy(buf, logp, sem).wait()


def solution(mesh):
    tp_size = mesh.shape["tp"]

    def per_device(hidden, lnf_gain, lnf_bias, emb_table, next_tok, eln_gain, eln_bias):
        rows, width = hidden.shape
        block = emb_table.shape[0] // tp_size
        T = 7 * LANES
        n = block // T
        S, S2, n0 = 3, 3, 5
        sizes = (1, 2, 5, 10, 10, 5, 1)
        groups, at = [], 1
        for size in sizes:
            groups.append((at, at + size))
            at += size
        head = (0, 3 * LANES, 5 * LANES, T)
        cfg = (n, T, block, S, S2, n0, float(width * tp_size), head, tuple(groups))
        vmem = pl.BlockSpec(memory_space=pltpu.VMEM)
        hbm = pl.BlockSpec(memory_space=pl.ANY)
        dma = pltpu.SemaphoreType.DMA
        z, lse, nin = pl.pallas_call(
            functools.partial(logits_kernel, cfg),
            out_shape=(
                pltpu.VMEM((rows, block), F32),
                pltpu.VMEM((8, LANES), F32),
                pltpu.VMEM((rows, width), BF16),
            ),
            in_specs=[hbm] * 7,
            out_specs=(vmem, vmem, vmem),
            scratch_shapes=[
                pltpu.VMEM((rows, width), BF16),
                pltpu.VMEM((1, width), F32),
                pltpu.VMEM((1, width), F32),
                pltpu.VMEM((1, rows), jnp.int32),
                pltpu.VMEM((1, width), F32),
                pltpu.VMEM((1, width), F32),
                dma((3,)),
                dma,
                dma((len(head) - 1,)),
                dma,
                pltpu.VMEM((rows, head[1]), F32),
                dma,
                pltpu.VMEM((rows, width), BF16),
                pltpu.VMEM((n, rows, T), F32),
                pltpu.VMEM((n, rows, T), F32),
                pltpu.VMEM((S2, rows, T), F32),
                pltpu.VMEM((S2, rows, T), F32),
                pltpu.VMEM((S, 2, T, width), BF16),
                pltpu.VMEM((rows, width), F32),
                pltpu.VMEM((rows, width), F32),
                pltpu.VMEM((rows, LANES), F32),
                pltpu.VMEM((rows, LANES), F32),
                pltpu.VMEM((8, LANES), F32),
                pltpu.VMEM((3, 8, LANES), F32),
                pltpu.VMEM((8, LANES), F32),
                pltpu.VMEM((3, 8, LANES), F32),
                pltpu.VMEM((8, LANES), F32),
                pltpu.VMEM((7, 8, LANES), F32),
                dma((S,)),
                dma((S2,)),
                dma((S2,)),
                dma,
                dma((len(groups),)),
                dma,
                dma,
                dma,
                dma,
                dma,
            ],
            compiler_params=pltpu.CompilerParams(
                collective_id=0, has_side_effects=True, vmem_limit_bytes=52 * 2**20),
        )(hidden, lnf_gain.reshape(1, width), lnf_bias.reshape(1, width), next_tok.reshape(1, rows),
          eln_gain.reshape(1, width), eln_bias.reshape(1, width), emb_table)
        logp, log_sum, next_in = pl.pallas_call(
            finish_kernel,
            out_shape=(
                jax.ShapeDtypeStruct((rows, block), F32),
                jax.ShapeDtypeStruct((1, rows), F32),
                jax.ShapeDtypeStruct((rows, width), BF16),
            ),
            in_specs=[vmem, vmem, vmem],
            out_specs=(hbm, hbm, hbm),
            scratch_shapes=[
                pltpu.VMEM((rows, block), F32), pltpu.VMEM((1, rows), F32), dma, dma((2,))],
            compiler_params=pltpu.CompilerParams(vmem_limit_bytes=20 * 2**20),
        )(z, lse, nin)
        return logp, log_sum.reshape(rows), next_in

    return jax.shard_map(
        per_device,
        mesh=mesh,
        in_specs=(P("dp", "tp"), P("tp"), P("tp"), P("vp", "tp"), P("dp"), P("tp"), P("tp")),
        out_specs=(P("dp", ("vp", "tp")), P("dp"), P("dp", "tp")),
        check_vma=False,
    )
```
